32 devices in a mesh: group: 2 (over y), tp: 16 (over z, x, core).
Axes of the slice: x: 2, y: 2, z: 4, core: 2. Of those that a mesh axis runs over, the one named last changes fastest.
Arguments:
- queries: bfloat16 [2, 8, 2, 8192], P('group', None, None, 'tp'), may hold values from -24 to 24
- new_keys: bfloat16 [2, 8, 2, 1024], P('group', None, None, 'tp'), may hold values from -16 to 16
- new_values: bfloat16 [2, 8, 2, 1024], P('group', None, None, 'tp'), may hold values from -24 to 24
- key_pages: bfloat16 [2, 1024, 16, 1024], P('group', 'tp'), may hold values from -16 to 16
- value_pages: bfloat16 [2, 1024, 16, 1024], P('group', 'tp'), may hold values from -24 to 24
- page_owner: int32 [2, 1024], P('group', 'tp'), may hold values from 0 to 8, as said below
- page_fill: int32 [2, 1024], P('group', 'tp'), may hold values from 0 to 16, as said below
- target_slot: int32 [2, 8], P('group'), may hold values from 0 to 8, as said below
- out_weight: bfloat16 [8192, 8192], P(None, 'tp'), may hold values from -0.0625 to 0.0625
Outputs:
- projected: bfloat16 [2, 8, 2, 8192], P('group', None, None, 'tp')
The draws below stay inside these ranges and needn't reach their ends.
Inputs may be any that keep to these rules, and one draw needn't show every extreme that they name: `page_owner`: the owning request slot, or 8 for a free page. Of each pair of groups g and g XOR (1) one is loaded (no free pages) and the other light; group 0 is light, and so is group 2 - 1 when 2 > 2. One device holds at most 16 pages of moving requests, and some device of every loaded group holds exactly 16. `page_fill`: 1 to 16 for a used page, 0 for a free one. `target_slot`: 8 for a request that stays. Every group has exactly one moving request; their slots in the partner group are distinct and own no pages there.
All inputs are finite; a program needn't handle non-finite values.
Results may differ from the reference program's by a relative error of at most 0.0065.
Values may be sent and summed in bfloat16 or wider, within the bound.
No kernel may reach another device: no remote copies, remote signals or barrier semaphores. Data moves between devices by JAX's collectives and lax.ppermute only.
A program may use at most 64 MiB of HBM per device.

```python
import math
import jax
import jax.numpy as jnp
from jax import lax

D = 8192
HEADS = 64
KVH = 8
HD = 128
PAGE = 16
STEPS = 2
CAP = 16
REQ = 8
PAGES_DEV = 64
MOVE = 1
GROUPS = 2
POOL = 1024


def distinct_order(key, shape):
    raw = jax.random.randint(key, shape, 0, 1 << 20)
    ranks = raw * shape[-1] + jnp.arange(shape[-1], dtype=jnp.int32)
    return jnp.argsort(ranks, axis=-1).astype(jnp.int32)


def layout(key):
    base = jax.random.fold_in(key, 4242)
    streams = jax.random.split(base, 11)
    half = GROUPS // 2
    tp_count = POOL // PAGES_DEV
    group_ids = jnp.arange(GROUPS, dtype=jnp.int32)
    pair_ids = group_ids % half
    partner_ids = jnp.bitwise_xor(group_ids, half).astype(jnp.int32)
    low_side = group_ids < half
    low_loaded = jax.random.randint(streams[0], (half,), 0, 2) == 1
    pair_range = jnp.arange(half, dtype=jnp.int32)
    low_loaded = jnp.where(pair_range == half - 1, True, low_loaded)
    low_loaded = jnp.where(pair_range == 0, False, low_loaded)
    loaded = jnp.where(low_side, low_loaded[pair_ids], jnp.logical_not(low_loaded[pair_ids]))
    orders = distinct_order(streams[1], (GROUPS, REQ))
    slot_ids = jnp.arange(REQ, dtype=jnp.int32)
    matched = (orders[:, :MOVE, None] == slot_ids[None, None, :]).astype(jnp.int32)
    receiving = orders[partner_ids][:, MOVE:2 * MOVE]
    slot_table = (REQ + jnp.sum(matched * (receiving[:, :, None] - REQ), axis=1)).astype(jnp.int32)
    device_shape = (GROUPS, tp_count, PAGES_DEV)
    position = jnp.arange(PAGES_DEV, dtype=jnp.int32)[None, None, :]
    mover_count = jax.random.randint(streams[3], (GROUPS, tp_count, 1), (CAP + 1) // 2, CAP + 1)
    full_device = jax.random.randint(streams[4], (GROUPS, 1, 1), 0, tp_count)
    mover_count = jnp.where(jnp.arange(tp_count, dtype=jnp.int32)[None, :, None] == full_device, CAP, mover_count)
    pick_mover = jax.random.randint(streams[5], device_shape, 0, MOVE)
    pick_stay = jax.random.randint(streams[6], device_shape, 2 * MOVE, REQ)
    rows = jnp.broadcast_to(orders[:, None, :], (GROUPS, tp_count, REQ))
    mover_owner = jnp.take_along_axis(rows, pick_mover, axis=2)
    stay_owner = jnp.take_along_axis(rows, pick_stay, axis=2)
    loaded_owner = jnp.where(position < mover_count, mover_owner, stay_owner)
    light_count = jax.random.randint(streams[7], (GROUPS, tp_count, 1), max(PAGES_DEV // 4, 1), PAGES_DEV // 2 + 1)
    light_owner = jnp.where(position < light_count, loaded_owner, REQ)
    owner_table = jnp.where(loaded[:, None, None], loaded_owner, light_owner)
    shuffle = distinct_order(streams[8], device_shape)
    owner_table = jnp.take_along_axis(owner_table, shuffle, axis=2).astype(jnp.int32)
    partial_fill = jax.random.randint(streams[9], device_shape, 1, PAGE + 1)
    partial_on = jax.random.randint(streams[10], device_shape, 0, 4) == 0
    fill_table = jnp.where(owner_table < REQ, jnp.where(partial_on, partial_fill, PAGE), 0).astype(jnp.int32)
    return (owner_table.reshape(GROUPS, POOL), fill_table.reshape(GROUPS, POOL), slot_table)


def draw_page_owner(key, part):
    return layout(key)[0]


def draw_page_fill(key, part):
    return layout(key)[1]


def draw_target_slot(key, part):
    return layout(key)[2]


def sign_table(key):
    signs = jax.random.randint(jax.random.fold_in(key, 777), (KVH, HD), 0, 2)
    return (2 * signs - 1).astype(jnp.float32)


def draw_queries(key, part):
    streams = jax.random.split(jax.random.fold_in(key, 101), 3)
    shape = (GROUPS, REQ, STEPS, HEADS, HD)
    flag_shape = (GROUPS, REQ, STEPS, HEADS, 1)
    noise = 1.5 * jax.random.truncated_normal(streams[0], -6.0, 6.0, shape, jnp.float32)
    aligned = jax.random.randint(streams[1], flag_shape, 0, 4) == 0
    levels = jnp.array([3.0, 5.0, 7.0], jnp.float32)
    strength = jnp.take(levels, jax.random.randint(streams[2], flag_shape, 0, 3))
    head_signs = jnp.repeat(sign_table(key), HEADS // KVH, axis=0)
    planted = strength * head_signs + 0.5 * noise
    result = jnp.where(aligned, planted, noise)
    return result.reshape(GROUPS, REQ, STEPS, D).astype(jnp.bfloat16)


def planted_keys(key, lead_shape, salt, shown_rate):
    streams = jax.random.split(jax.random.fold_in(key, salt), 3)
    full_shape = lead_shape + (KVH, HD)
    flag_shape = lead_shape + (KVH, 1)
    noise = jax.random.truncated_normal(streams[0], -6.0, 6.0, full_shape, jnp.float32)
    chosen = jax.random.randint(streams[1], flag_shape, 0, shown_rate) == 0
    reach = jax.random.uniform(streams[2], flag_shape, jnp.float32, 1.5, 3.5)
    planted = reach * sign_table(key) + 0.5 * noise
    result = jnp.where(chosen, planted, noise)
    return result.reshape(lead_shape + (KVH * HD,)).astype(jnp.bfloat16)


def draw_key_pages(key, part):
    return planted_keys(key, (GROUPS, POOL, PAGE), 202, 64)


def draw_new_keys(key, part):
    return planted_keys(key, (GROUPS, REQ, STEPS), 303, 2)


def block_scale(key, shape, shards, low, high):
    def one(axis_at, blocks):
        steps = jax.random.uniform(jax.random.fold_in(jax.random.fold_in(key, 6), axis_at), (blocks,), jnp.float32, low / len(shards), high / len(shards))
        return jnp.repeat(jnp.exp(steps), shape[axis_at] // blocks).reshape((-1,) + (1,) * (len(shape) - axis_at - 1))

    level = one(*shards[0])
    for cut in shards[1:]:
        level = level * one(*cut)
    return level


def gaussian(key, extent, width, most, cuts=(), kind=jnp.bfloat16):
    entries = jax.random.normal(key, extent, jnp.float32) * width
    if len(cuts) > 0:
        entries = block_scale(key, extent, cuts, -0.22, 0.18) * entries
    return jnp.clip(entries, min=-most, max=most).astype(kind)


def setup_inputs(seed: int = 0) -> dict:
    key_list = jax.random.split(jax.random.key(seed), 10)
    queries = draw_queries(jax.random.fold_in(key_list[9], 71), 0)
    new_keys = draw_new_keys(jax.random.fold_in(key_list[9], 71), 0)
    new_values = gaussian(key_list[2], (GROUPS, REQ, STEPS, KVH * HD), 4.0, 24.0, ((0, 2), (3, 16)))
    key_pages = draw_key_pages(jax.random.fold_in(key_list[9], 71), 0)
    value_pages = gaussian(key_list[4], (GROUPS, POOL, PAGE, KVH * HD), 4.0, 24.0, ((0, 2), (1, 16)))
    page_owner = draw_page_owner(jax.random.fold_in(key_list[9], 71), 0)
    page_fill = draw_page_fill(jax.random.fold_in(key_list[9], 71), 0)
    target_slot = draw_target_slot(jax.random.fold_in(key_list[9], 71), 0)
    out_weight = gaussian(key_list[8], (D, D), D ** -0.5, 0.0625, ((1, 16),))
    return dict(queries=queries, new_keys=new_keys, new_values=new_values, key_pages=key_pages, value_pages=value_pages, page_owner=page_owner, page_fill=page_fill, target_slot=target_slot, out_weight=out_weight)


neg_big = -1e+30

def merge_states(first, second):
    largest = jnp.maximum(first[0], second[0])
    scale_first = jnp.exp(first[0] - largest)
    scale_second = jnp.exp(second[0] - largest)
    return (largest, first[1] * scale_first + second[1] * scale_second, first[2] * scale_first[..., None] + second[2] * scale_second[..., None])

def page_states(query_rows, key_block, value_block, owner_rows, fill_counts, row_count):
    page_count = key_block.shape[0]
    step_count = query_rows.shape[1]
    group_size = HEADS // KVH
    scale_factor = 1.0 / math.sqrt(HD)
    clipped = jnp.clip(owner_rows, 0, row_count - 1).astype(jnp.int32)
    query_page = jnp.take(query_rows, clipped, axis=0).reshape(page_count, step_count, KVH, group_size, HD).astype(jnp.float32)
    key_page = key_block.reshape(page_count, PAGE, KVH, HD).astype(jnp.float32)
    value_page = value_block.reshape(page_count, PAGE, KVH, HD).astype(jnp.float32)
    scores = jnp.einsum('psgjd,ptgd->psgjt', query_page, key_page) * scale_factor
    live_token = (owner_rows < row_count)[:, None] & (lax.broadcasted_iota(jnp.int32, (page_count, PAGE), 1) < fill_counts[:, None])
    token_mask = live_token[:, None, None, None, :]
    scores = jnp.where(token_mask, scores, neg_big)
    page_top = lax.optimization_barrier(jnp.max(scores, axis=4)).reshape(page_count, step_count * HEADS)
    member = owner_rows[None, :] == lax.broadcasted_iota(jnp.int32, (row_count, page_count), 0)
    row_top = lax.optimization_barrier(jnp.max(jnp.where(member[:, :, None], page_top[None], neg_big), axis=1))
    top_page = jnp.take(row_top, clipped, axis=0).reshape(page_count, step_count, KVH, group_size, 1)
    weights = jnp.where(token_mask, jnp.exp(scores - top_page), 0.0).astype(jnp.bfloat16).astype(jnp.float32)
    weighted = jnp.einsum('psgjt,ptgd->psgjd', weights, value_page).reshape(page_count, step_count, HEADS, HD)
    weight_sum = lax.optimization_barrier(jnp.sum(weights, axis=4)).reshape(page_count, step_count, HEADS)
    row_sum = jax.ops.segment_sum(weight_sum, owner_rows, num_segments=row_count + 1)[:row_count]
    row_acc = jax.ops.segment_sum(weighted, owner_rows, num_segments=row_count + 1)[:row_count]
    return (row_top.reshape(row_count, step_count, HEADS), row_sum, row_acc)

def new_token_states(query_heads, key_rows, value_rows, head_kv):
    row_count = key_rows.shape[0]
    step_count = key_rows.shape[1]
    scale_factor = 1.0 / math.sqrt(HD)
    key_heads = jnp.take(key_rows.reshape(row_count, step_count, KVH, HD), head_kv, axis=2).astype(jnp.float32)
    value_heads = jnp.take(value_rows.reshape(row_count, step_count, KVH, HD), head_kv, axis=2).astype(jnp.float32)
    scores = jnp.einsum('rshd,ruhd->rshu', query_heads.astype(jnp.float32), key_heads) * scale_factor
    causal = (lax.broadcasted_iota(jnp.int32, (step_count, step_count), 1) <= lax.broadcasted_iota(jnp.int32, (step_count, step_count), 0))[None, :, None, :]
    scores = jnp.where(causal, scores, neg_big)
    largest = lax.optimization_barrier(jnp.max(scores, axis=3))
    weights = jnp.where(causal, jnp.exp(scores - largest[..., None]), 0.0)
    return (largest, lax.optimization_barrier(jnp.sum(weights, axis=3)), jnp.einsum('rshu,ruhd->rshd', weights, value_heads))

def flatten_rows(member_array):
    return member_array.reshape((member_array.shape[0] * member_array.shape[1],) + member_array.shape[2:])

def reference(queries, new_keys, new_values, key_pages, value_pages, page_owner, page_fill, target_slot, out_weight):
    groups = queries.shape[0]
    row_count = queries.shape[1]
    step_count = queries.shape[2]
    partner = jnp.bitwise_xor(jnp.arange(groups, dtype=jnp.int32), groups // 2).astype(jnp.int32)

    def per_group(group_index):
        owners = page_owner[group_index]
        slot_targets = target_slot[group_index]
        clipped = jnp.clip(owners, 0, row_count - 1).astype(jnp.int32)
        page_target = jnp.take(slot_targets, clipped)
        occupied = owners < row_count
        moving = occupied & (page_target < row_count)
        local_rows = jnp.where(occupied, jnp.where(moving, row_count + page_target, owners), 2 * row_count).astype(jnp.int32)
        query_rows = jnp.concatenate([queries[group_index], queries[partner[group_index]]], axis=0)
        return page_states(query_rows, key_pages[group_index], value_pages[group_index], local_rows, page_fill[group_index], 2 * row_count)
    all_states = lax.map(per_group, jnp.arange(groups, dtype=jnp.int32))
    own_part = tuple((member_array[:, :row_count] for member_array in all_states))
    arrived = tuple((member_array[partner][:, row_count:] for member_array in all_states))
    cache_state = merge_states(own_part, arrived)
    cache_flat = tuple((flatten_rows(member_array) for member_array in cache_state))
    head_kv = (jnp.arange(HEADS, dtype=jnp.int32) // (HEADS // KVH)).astype(jnp.int32)
    query_heads = flatten_rows(queries).reshape(groups * row_count, step_count, HEADS, HD)
    new_terms = new_token_states(query_heads, flatten_rows(new_keys), flatten_rows(new_values), head_kv)
    finished = merge_states(cache_flat, new_terms)
    attention = (finished[2] / finished[1][..., None]).astype(jnp.bfloat16).reshape(groups * row_count * step_count, HEADS * HD)
    projected = jnp.dot(attention, out_weight, preferred_element_type=jnp.float32).astype(jnp.bfloat16)
    return projected.reshape(groups, row_count, step_count, HEADS * HD)
```

```python
import math

import jax
import jax.numpy as jnp
from jax import lax
from jax.experimental import pallas as pl
from jax.experimental.pallas import tpu as pltpu
from jax.sharding import PartitionSpec as P

HEADS = 64
KVH = 8
HD = 128
PAGE = 16
NEG = -1e30
FLOOR = -1e29
SCALE = 1.0 / math.sqrt(HD) * math.log2(math.e)
MOVED_LANE = 64
GS = HEADS // KVH


def dot(a, b, contract):
    return lax.dot_general(a, b, ((contract), ((), ())), preferred_element_type=jnp.float32)


def iota(shape, axis):
    return lax.broadcasted_iota(jnp.int32, shape, axis)


def attend_kernel(
    chips, info, slots, owner, fill, own, other, keys, values, out, bias_own, bias_moved
):
    row_steps = own.shape[1]
    rows = slots.shape[0]
    steps = row_steps // rows
    features = HEADS // (2 * chips) * HD
    local_heads = features // HD
    kv_part = (own.shape[2] - features) // 2
    per_kv = chips // KVH
    tokens = keys.shape[0]
    half_rs = row_steps // 2
    half = info[0]
    core = info[1]
    first = info[2]
    mover = jnp.int32(0)
    target = jnp.int32(0)
    for r in range(rows):
        leaves = slots[r] < rows
        mover = jnp.where(leaves, r, mover)
        target = jnp.where(leaves, slots[r], target)

    pages = owner.shape[1]
    spread = (iota((pages, tokens), 1) // PAGE == iota((pages, tokens), 0)).astype(jnp.bfloat16)
    table = jnp.concatenate([owner[...], fill[...]], axis=0).astype(jnp.float32)
    table = jnp.concatenate([table] * 4, axis=0).astype(jnp.bfloat16)
    by_token = dot(table, spread, ((1,), (0,)))
    owner_tok = by_token[0:1].astype(jnp.int32)
    fill_tok = by_token[1:2].astype(jnp.int32)
    live = iota((1, tokens), 1) % PAGE < fill_tok
    token_row = jnp.where(live, owner_tok, rows)
    stay_row = jnp.where(token_row == mover, rows, token_row)
    bias_own[...] = jnp.where(iota((row_steps, tokens), 0) // steps == stay_row, 0.0, NEG)
    bias_moved[...] = jnp.broadcast_to(jnp.where(token_row == mover, 0.0, NEG), bias_moved.shape)

    rs_ids = iota((row_steps, row_steps), 0)
    new_ids = iota((row_steps, row_steps), 1)
    new_live = (rs_ids // steps == new_ids // steps) & (new_ids % steps <= rs_ids % steps)
    bias_new = jnp.where(new_live & (first == 1), 0.0, NEG)
    moved_rows = GS * steps
    wide = GS * row_steps
    pick_ids = iota((moved_rows, wide), 0)
    pick = (
        iota((moved_rows, wide), 1)
        == (pick_ids // steps) * row_steps + target * steps + pick_ids % steps
    ).astype(jnp.bfloat16)
    lane = iota((half_rs, HD), 1)
    target_f = target.astype(jnp.float32)

    def per_head(g, carry):
        tiles, partner_tiles, new_k, new_v = [], [], [], []
        for source in (own, other):
            for kl in range(per_kv):
                mine = source[half * chips + g * per_kv + kl]
                theirs = source[(1 - half) * chips + g * per_kv + kl]
                for j in range(local_heads):
                    tiles.append(mine[:, j * HD : (j + 1) * HD])
                    partner_tiles.append(theirs[:, j * HD : (j + 1) * HD])
                new_k.append(mine[:, features : features + kv_part])
                new_v.append(mine[:, features + kv_part :])

        def in_order(parts):
            mine, theirs = parts[:per_kv], parts[per_kv:]
            a = [x for pair in zip(mine, theirs) for x in pair]
            b = [x for pair in zip(theirs, mine) for x in pair]
            return jnp.where(
                core == 0,
                jnp.concatenate(a, axis=1).astype(jnp.float32),
                jnp.concatenate(b, axis=1).astype(jnp.float32),
            ).astype(jnp.bfloat16)

        moved_q = dot(pick, jnp.concatenate(partner_tiles, axis=0), ((1,), (0,)))
        q = jnp.concatenate(tiles + [moved_q.astype(jnp.bfloat16)], axis=0)
        at = pl.ds(pl.multiple_of(g * HD, HD), HD)
        k = keys[:, at]
        v = values[:, at]
        scores = dot(q, k, ((1,), (1,))) * SCALE
        bias = jnp.concatenate([bias_own[...]] * GS + [bias_moved[...]], axis=0)
        scores = scores + bias
        new_scores = dot(q[:wide], in_order(new_k), ((1,), (1,))) * SCALE
        new_scores = new_scores + jnp.concatenate([bias_new] * GS, axis=0)
        new_scores = jnp.concatenate(
            [new_scores, jnp.full((moved_rows, row_steps), NEG, jnp.float32)], axis=0
        )
        top = jnp.maximum(
            jnp.max(scores, axis=1, keepdims=True), jnp.max(new_scores, axis=1, keepdims=True)
        )
        top = jnp.maximum(top, FLOOR).astype(jnp.bfloat16).astype(jnp.float32)
        p = jnp.exp2(scores - top).astype(jnp.bfloat16)
        pn = jnp.exp2(new_scores - top).astype(jnp.bfloat16)
        total = jnp.sum(p.astype(jnp.float32), axis=1, keepdims=True) + jnp.sum(
            pn.astype(jnp.float32), axis=1, keepdims=True
        )
        acc = dot(p, v, ((1,), (0,))) + dot(pn, in_order(new_v), ((1,), (0,)))
        high = total.astype(jnp.bfloat16).astype(jnp.float32)
        low = total - high

        for side in range(2):
            for kl in range(per_kv):
                dest = 2 * (g * per_kv + kl) + jnp.where(side == 0, core, 1 - core)
                t0 = (side * per_kv + kl) * local_heads
                at_moved = slice(wide + t0 * steps, wide + (t0 + local_heads) * steps)
                moved_acc = acc[at_moved]
                short = half_rs - local_heads * steps

                def filled(x):
                    if short == 0:
                        return x
                    return jnp.concatenate([x, jnp.zeros((short, x.shape[1]), x.dtype)], axis=0)

                for h in range(2):
                    parts = [
                        acc[(t0 + j) * row_steps + h * half_rs :][:half_rs]
                        for j in range(local_heads)
                    ]
                    aux = jnp.where(lane == MOVED_LANE, filled(top[at_moved]), 0.0)
                    aux = jnp.where(lane == MOVED_LANE + 1, filled(high[at_moved]), aux)
                    aux = jnp.where(lane == MOVED_LANE + 2, filled(low[at_moved]), aux)
                    aux = jnp.where(lane == MOVED_LANE + 3, target_f, aux)
                    for j in range(local_heads):
                        rows_at = slice(
                            (t0 + j) * row_steps + h * half_rs,
                            (t0 + j) * row_steps + (h + 1) * half_rs,
                        )
                        aux = jnp.where(lane == j, top[rows_at], aux)
                        aux = jnp.where(lane == local_heads + j, high[rows_at], aux)
                        aux = jnp.where(lane == 2 * local_heads + j, low[rows_at], aux)
                    block = jnp.concatenate(parts + [filled(moved_acc), aux], axis=0)
                    out[h, dest] = block.astype(jnp.bfloat16)
        return carry

    lax.fori_loop(0, KVH, per_head, 0)


def reduce_kernel(chips, steps, info, parts, out):
    sources = 2 * chips
    half_rs = out.shape[2]
    local_heads = out.shape[3] // HD
    half = info[0]
    span = half_rs * local_heads
    row_ids = iota((half_rs, 1), 0)
    for g in range(2):
        blocks = [parts[(1 - g) * sources + t].astype(jnp.float32) for t in range(sources)]
        aux = [b[span + half_rs :] for b in blocks]
        column = [a[:, MOVED_LANE : MOVED_LANE + 1] for a in aux]
        top = column[0]
        for c in column[1:]:
            top = jnp.maximum(top, c)
        moved_sum = jnp.zeros((half_rs, 1), jnp.float32)
        moved_acc = jnp.zeros((half_rs, HD), jnp.float32)
        for t in range(sources):
            w = jnp.exp2(column[t] - top)
            a = aux[t]
            moved_sum += w * (
                a[:, MOVED_LANE + 1 : MOVED_LANE + 2] + a[:, MOVED_LANE + 2 : MOVED_LANE + 3]
            )
            moved_acc += w * blocks[t][span : span + half_rs]
        moved_top = top
        slot = aux[0][:, MOVED_LANE + 3 : MOVED_LANE + 4]
        mine = (half_rs // steps * half + row_ids // steps).astype(jnp.float32) == slot
        blocks = [parts[g * sources + t].astype(jnp.float32) for t in range(sources)]
        aux = [b[span + half_rs :] for b in blocks]
        done = []
        for j in range(local_heads):

            def placed(x):
                y = jnp.broadcast_to(x[j * steps : j * steps + 1], (half_rs, x.shape[1]))
                for s in range(1, steps):
                    z = jnp.broadcast_to(x[j * steps + s : j * steps + s + 1], y.shape)
                    y = jnp.where(row_ids % steps == s, z, y)
                return y

            m_in = jnp.where(mine, placed(moved_top), FLOOR)
            column = [a[:, j : j + 1] for a in aux]
            top = m_in
            for c in column:
                top = jnp.maximum(top, c)
            w = jnp.where(mine, jnp.exp2(m_in - top), 0.0)
            total = w * placed(moved_sum)
            acc = w * placed(moved_acc)
            for t in range(sources):
                w = jnp.exp2(column[t] - top)
                a = aux[t]
                total += w * (
                    a[:, local_heads + j : local_heads + j + 1]
                    + a[:, 2 * local_heads + j : 2 * local_heads + j + 1]
                )
                acc += w * blocks[t][j * half_rs : (j + 1) * half_rs]
            done.append(acc / total)
        result = jnp.concatenate(done, axis=1).astype(jnp.bfloat16)
        for k in range(chips):
            out[g, k] = result


def project_kernel(chips, info, own, other, weight, out):
    core = info[1]
    acc = None
    for side, source in enumerate((own, other)):
        which = core if side == 0 else 1 - core
        for k in range(chips):
            x = jnp.concatenate([source[k], source[chips + k]], axis=0)
            part = dot(x, weight[2 * k + which], ((1,), (0,)))
            acc = part if acc is None else acc + part
    out[...] = acc.astype(jnp.bfloat16)


SMEM = pl.BlockSpec(memory_space=pltpu.SMEM)
VMEM = pl.BlockSpec(memory_space=pltpu.VMEM)


def per_device_of(groups, width):
    chips = width // 2
    apart = groups // 2
    same_core = [
        [(g + h * apart) * width + 2 * k + c for h in range(2) for k in range(chips)]
        for g in range(apart)
        for c in range(2)
    ]
    paired = [
        [(g + h * apart) * width + t for h in range(2) for t in range(width)] for g in range(apart)
    ]
    across = [(t, t ^ 1) for t in range(width)]
    both = ("group", "tp")

    def exchange(x, members):
        return lax.all_to_all(x, both, 0, 0, axis_index_groups=members)

    def per_device(
        queries,
        new_keys,
        new_values,
        key_pages,
        value_pages,
        page_owner,
        page_fill,
        target_slot,
        out_weight,
    ):
        rows, steps, features = queries.shape[1:]
        local_heads = features // HD
        row_steps = rows * steps
        half_rs = row_steps // 2
        pages = key_pages.shape[1]
        tokens = pages * PAGE
        place = lax.axis_index("tp")
        half = lax.axis_index("group") // apart
        info = jnp.stack([half, place % 2, (place == 0).astype(jnp.int32)]).astype(jnp.int32)

        packed = jnp.concatenate([queries[0], new_keys[0], new_values[0]], axis=2)
        packed = packed.reshape(1, row_steps, packed.shape[2])
        sent = jnp.broadcast_to(packed, (2 * chips,) + packed.shape[1:])
        own = exchange(sent, same_core)
        other = lax.ppermute(own, "tp", across)

        block_rows = half_rs * local_heads + 2 * half_rs
        states = pl.pallas_call(
            lambda *refs: attend_kernel(chips, *refs),
            out_shape=jax.ShapeDtypeStruct((2, width, block_rows, HD), jnp.bfloat16),
            in_specs=[SMEM, SMEM] + [VMEM] * 6,
            out_specs=VMEM,
            scratch_shapes=[
                pltpu.VMEM((row_steps, tokens), jnp.float32),
                pltpu.VMEM((GS * steps, tokens), jnp.float32),
            ],
            name="attend",
        )(
            info,
            target_slot[0],
            page_owner,
            page_fill,
            own,
            other,
            key_pages.reshape(tokens, key_pages.shape[3]),
            value_pages.reshape(tokens, value_pages.shape[3]),
        )
        arrived = exchange(states.reshape(2 * width, block_rows, HD), paired)
        finished = pl.pallas_call(
            lambda *refs: reduce_kernel(chips, steps, *refs),
            out_shape=jax.ShapeDtypeStruct((2, chips, half_rs, features), jnp.bfloat16),
            in_specs=[SMEM, VMEM],
            out_specs=VMEM,
            name="reduce",
        )(info, arrived)
        own = exchange(finished.reshape(2 * chips, half_rs, features), same_core)
        other = lax.ppermute(own, "tp", across)
        projected = pl.pallas_call(
            lambda *refs: project_kernel(chips, *refs),
            out_shape=jax.ShapeDtypeStruct((row_steps, out_weight.shape[1]), jnp.bfloat16),
            in_specs=[SMEM, VMEM, VMEM, VMEM],
            out_specs=VMEM,
            name="project",
        )(info, own, other, out_weight.reshape(width, features, out_weight.shape[1]))
        return projected.reshape(1, rows, steps, out_weight.shape[1])

    return per_device


def solution(mesh):
    placed = (
        P("group", None, None, "tp"),
        P("group", None, None, "tp"),
        P("group", None, None, "tp"),
        P("group", "tp", None, None),
        P("group", "tp", None, None),
        P("group", "tp"),
        P("group", "tp"),
        P("group", None),
        P(None, "tp"),
    )
    return jax.shard_map(
        per_device_of(mesh.shape["group"], mesh.shape["tp"]),
        mesh=mesh,
        in_specs=placed,
        out_specs=P("group", None, None, "tp"),
        check_vma=False,
    )
```

```python
import math

import jax
import jax.numpy as jnp
from jax import lax
from jax.experimental import pallas as pl
from jax.experimental.pallas import tpu as pltpu
from jax.sharding import PartitionSpec as P

HEADS = 64
KVH = 8
HD = 128
PAGE = 16
NEG = -1e30
FLOOR = -1e29
SCALE = 1.0 / math.sqrt(HD) * math.log2(math.e)
MOVED_LANE = 64
TARGET_LANE = 127
GS = HEADS // KVH


def dot(a, b, contract):
    return lax.dot_general(a, b, ((contract), ((), ())), preferred_element_type=jnp.float32)


def iota(shape, axis):
    return lax.broadcasted_iota(jnp.int32, shape, axis)


def pack_kernel(queries, new_keys, new_values, out):
    row_steps = out.shape[1]
    row = jnp.concatenate(
        [x[...].reshape(row_steps, x.shape[2]) for x in (queries, new_keys, new_values)], axis=1
    )
    for i in range(out.shape[0]):
        out[i] = row


def sums_of(aux, local_heads):
    high = pltpu.roll(aux, HD - local_heads, 1)
    return high + pltpu.roll(aux, HD - 2 * local_heads, 1)


def split(total):
    high = total.astype(jnp.bfloat16).astype(jnp.float32)
    return high, total - high


def attend_kernel(
    chips, info, slots, owner, fill, own, other, keys, values, keep, send, bias_own, bias_moved
):
    row_steps = own.shape[1]
    rows = slots.shape[0]
    steps = row_steps // rows
    features = HEADS // (2 * chips) * HD
    local_heads = features // HD
    kv_part = (own.shape[2] - features) // 2
    per_kv = chips // KVH
    tokens = keys.shape[0]
    half_rs = row_steps // 2
    half = info[0]
    core = info[1]
    first = info[2]
    mover = jnp.int32(0)
    target = jnp.int32(0)
    for r in range(rows):
        leaves = slots[r] < rows
        mover = jnp.where(leaves, r, mover)
        target = jnp.where(leaves, slots[r], target)

    pages = owner.shape[1]
    spread = (iota((pages, tokens), 1) // PAGE == iota((pages, tokens), 0)).astype(jnp.bfloat16)
    table = jnp.concatenate([owner[...], fill[...]], axis=0).astype(jnp.float32)
    table = jnp.concatenate([table] * 4, axis=0).astype(jnp.bfloat16)
    by_token = dot(table, spread, ((1,), (0,)))
    owner_tok = by_token[0:1].astype(jnp.int32)
    fill_tok = by_token[1:2].astype(jnp.int32)
    live = iota((1, tokens), 1) % PAGE < fill_tok
    token_row = jnp.where(live, owner_tok, rows)
    stay_row = jnp.where(token_row == mover, rows, token_row)
    bias_own[...] = jnp.where(iota((row_steps, tokens), 0) // steps == stay_row, 0.0, NEG)
    bias_moved[...] = jnp.broadcast_to(jnp.where(token_row == mover, 0.0, NEG), bias_moved.shape)

    rs_ids = iota((row_steps, row_steps), 0)
    new_ids = iota((row_steps, row_steps), 1)
    new_live = (rs_ids // steps == new_ids // steps) & (new_ids % steps <= rs_ids % steps)
    bias_new = jnp.where(new_live & (first == 1), 0.0, NEG)
    moved_rows = GS * steps
    wide = GS * row_steps
    pick_ids = iota((moved_rows, wide), 0)
    pick = (
        iota((moved_rows, wide), 1)
        == (pick_ids // steps) * row_steps + target * steps + pick_ids % steps
    ).astype(jnp.bfloat16)
    lane = iota((half_rs, HD), 1)
    target_f = target.astype(jnp.float32)

    def per_head(g, carry):
        tiles, partner_tiles, new_k, new_v = [], [], [], []
        for source in (own, other):
            for kl in range(per_kv):
                mine = source[half * chips + g * per_kv + kl]
                theirs = source[(1 - half) * chips + g * per_kv + kl]
                for j in range(local_heads):
                    tiles.append(mine[:, j * HD : (j + 1) * HD])
                    partner_tiles.append(theirs[:, j * HD : (j + 1) * HD])
                new_k.append(mine[:, features : features + kv_part])
                new_v.append(mine[:, features + kv_part :])

        def in_order(parts):
            mine, theirs = parts[:per_kv], parts[per_kv:]
            a = [x for pair in zip(mine, theirs) for x in pair]
            b = [x for pair in zip(theirs, mine) for x in pair]
            return jnp.where(
                core == 0,
                jnp.concatenate(a, axis=1).astype(jnp.float32),
                jnp.concatenate(b, axis=1).astype(jnp.float32),
            ).astype(jnp.bfloat16)

        moved_q = dot(pick, jnp.concatenate(partner_tiles, axis=0), ((1,), (0,)))
        q = jnp.concatenate(tiles + [moved_q.astype(jnp.bfloat16)], axis=0)
        at = pl.ds(pl.multiple_of(g * HD, HD), HD)
        k = keys[:, at]
        v = values[:, at]
        scores = dot(q, k, ((1,), (1,))) * SCALE
        bias = jnp.concatenate([bias_own[...]] * GS + [bias_moved[...]], axis=0)
        scores = scores + bias
        new_scores = dot(q[:wide], in_order(new_k), ((1,), (1,))) * SCALE
        new_scores = new_scores + jnp.concatenate([bias_new] * GS, axis=0)
        new_scores = jnp.concatenate(
            [new_scores, jnp.full((moved_rows, row_steps), NEG, jnp.float32)], axis=0
        )
        top = jnp.maximum(
            jnp.max(scores, axis=1, keepdims=True), jnp.max(new_scores, axis=1, keepdims=True)
        )
        top = jnp.maximum(top, FLOOR).astype(jnp.bfloat16).astype(jnp.float32)
        p = jnp.exp2(scores - top).astype(jnp.bfloat16)
        pn = jnp.exp2(new_scores - top).astype(jnp.bfloat16)
        total = jnp.sum(p.astype(jnp.float32), axis=1, keepdims=True) + jnp.sum(
            pn.astype(jnp.float32), axis=1, keepdims=True
        )
        acc = dot(p, v, ((1,), (0,))) + dot(pn, in_order(new_v), ((1,), (0,)))
        high, low = split(total)

        for side in range(2):
            for kl in range(per_kv):
                t0 = (side * per_kv + kl) * local_heads
                at_moved = slice(wide + t0 * steps, wide + (t0 + local_heads) * steps)
                moved_acc = acc[at_moved]
                short = half_rs - local_heads * steps

                def filled(x):
                    if short == 0:
                        return x
                    return jnp.concatenate([x, jnp.zeros((short, x.shape[1]), x.dtype)], axis=0)

                for h in range(2):
                    parts = [
                        acc[(t0 + j) * row_steps + h * half_rs :][:half_rs]
                        for j in range(local_heads)
                    ]
                    aux = jnp.where(lane == MOVED_LANE, filled(top[at_moved]), 0.0)
                    aux = jnp.where(lane == MOVED_LANE + local_heads, filled(high[at_moved]), aux)
                    aux = jnp.where(lane == MOVED_LANE + 2 * local_heads, filled(low[at_moved]), aux)
                    aux = jnp.where(lane == TARGET_LANE, target_f, aux)
                    for j in range(local_heads):
                        rows_at = slice(
                            (t0 + j) * row_steps + h * half_rs,
                            (t0 + j) * row_steps + (h + 1) * half_rs,
                        )
                        aux = jnp.where(lane == j, top[rows_at], aux)
                        aux = jnp.where(lane == local_heads + j, high[rows_at], aux)
                        aux = jnp.where(lane == 2 * local_heads + j, low[rows_at], aux)
                    block = jnp.concatenate(parts + [filled(moved_acc), aux], axis=0)
                    dest = keep if side == 0 else send
                    dest[h, g * per_kv + kl] = block.astype(jnp.bfloat16)
        return carry

    lax.fori_loop(0, KVH, per_head, 0)


def merge_kernel(local_heads, first, second, out):
    half_rs = (first.shape[2]) // (local_heads + 2)
    span = half_rs * local_heads
    lane = iota((half_rs, HD), 1)
    for h in range(first.shape[0]):
        for k in range(first.shape[1]):
            a = first[h, k].astype(jnp.float32)
            b = second[h, k].astype(jnp.float32)
            aux_a, aux_b = a[span + half_rs :], b[span + half_rs :]
            top = jnp.maximum(aux_a, aux_b)
            wa = jnp.exp2(aux_a - top)
            wb = jnp.exp2(aux_b - top)
            total = wa * sums_of(aux_a, local_heads) + wb * sums_of(aux_b, local_heads)
            high, low = split(total)
            is_top = (lane < local_heads) | (lane >= MOVED_LANE)
            is_top = is_top & (lane < MOVED_LANE + local_heads) | (lane == TARGET_LANE)
            high = pltpu.roll(high, local_heads, 1)
            low = pltpu.roll(low, 2 * local_heads, 1)
            part = lane % MOVED_LANE // local_heads
            aux = jnp.where(is_top, top, jnp.where(part == 1, high, low))
            parts = []
            for j in range(local_heads + 1):
                at = j if j < local_heads else MOVED_LANE
                rows = slice(j * half_rs, (j + 1) * half_rs)
                parts.append(wa[:, at : at + 1] * a[rows] + wb[:, at : at + 1] * b[rows])
            out[h, k] = jnp.concatenate(parts + [aux], axis=0).astype(jnp.bfloat16)


def reduce_kernel(chips, steps, info, parts, out):
    half_rs = out.shape[2]
    local_heads = out.shape[3] // HD
    half = info[0]
    span = half_rs * local_heads
    row_ids = iota((half_rs, 1), 0)
    tops, sums, accs = [], [], []
    for g in range(2):
        aux = [
            parts[g * chips + k, span + half_rs :].astype(jnp.float32) for k in range(chips)
        ]
        top = aux[0]
        for a in aux[1:]:
            top = jnp.maximum(top, a)
        total = None
        acc = [None] * (local_heads + 1)
        for k in range(chips):
            w = jnp.exp2(aux[k] - top)
            part = w * sums_of(aux[k], local_heads)
            total = part if total is None else total + part
            for j in range(local_heads + 1):
                at = j if j < local_heads else MOVED_LANE
                block = parts[g * chips + k, j * half_rs : (j + 1) * half_rs]
                part = w[:, at : at + 1] * block.astype(jnp.float32)
                acc[j] = part if acc[j] is None else acc[j] + part
        tops.append(top)
        sums.append(total)
        accs.append(acc)
    for g in range(2):
        slot = tops[1 - g][:, TARGET_LANE : TARGET_LANE + 1]
        mine = (half_rs // steps * half + row_ids // steps).astype(jnp.float32) == slot
        moved_top = tops[1 - g][:, MOVED_LANE : MOVED_LANE + 1]
        moved_sum = sums[1 - g][:, MOVED_LANE : MOVED_LANE + 1]
        moved_acc = accs[1 - g][local_heads]
        done = []
        for j in range(local_heads):

            def placed(x):
                y = jnp.broadcast_to(x[j * steps : j * steps + 1], (half_rs, x.shape[1]))
                for s in range(1, steps):
                    z = jnp.broadcast_to(x[j * steps + s : j * steps + s + 1], y.shape)
                    y = jnp.where(row_ids % steps == s, z, y)
                return y

            own_top = tops[g][:, j : j + 1]
            in_top = jnp.where(mine, placed(moved_top), FLOOR)
            top = jnp.maximum(own_top, in_top)
            w_own = jnp.exp2(own_top - top)
            w_in = jnp.where(mine, jnp.exp2(in_top - top), 0.0)
            total = w_own * sums[g][:, j : j + 1] + w_in * placed(moved_sum)
            done.append((w_own * accs[g][j] + w_in * placed(moved_acc)) / total)
        result = jnp.concatenate(done, axis=1).astype(jnp.bfloat16)
        for k in range(chips):
            out[g, k] = result


def project_kernel(chips, info, own, other, weight, out):
    core = info[1]
    acc = None
    for side, source in enumerate((own, other)):
        which = core if side == 0 else 1 - core
        for k in range(chips):
            x = jnp.concatenate([source[k], source[chips + k]], axis=0)
            part = dot(x, weight[2 * k + which], ((1,), (0,)))
            acc = part if acc is None else acc + part
    out[...] = acc.astype(jnp.bfloat16).reshape(out.shape)


def limit(mib):
    return pltpu.CompilerParams(vmem_limit_bytes=mib << 20)


SMEM = pl.BlockSpec(memory_space=pltpu.SMEM)
VMEM = pl.BlockSpec(memory_space=pltpu.VMEM)


def per_device_of(groups, width):
    chips = width // 2
    apart = groups // 2
    same_core = [
        [(g + h * apart) * width + 2 * k + c for h in range(2) for k in range(chips)]
        for g in range(apart)
        for c in range(2)
    ]
    across = [(t, t ^ 1) for t in range(width)]
    both = ("group", "tp")

    def exchange(x, members):
        return lax.all_to_all(x, both, 0, 0, axis_index_groups=members)

    def per_device(
        queries,
        new_keys,
        new_values,
        key_pages,
        value_pages,
        page_owner,
        page_fill,
        target_slot,
        out_weight,
    ):
        rows, steps, features = queries.shape[1:]
        local_heads = features // HD
        row_steps = rows * steps
        half_rs = row_steps // 2
        pages = key_pages.shape[1]
        tokens = pages * PAGE
        place = lax.axis_index("tp")
        half = lax.axis_index("group") // apart
        info = jnp.stack([half, place & 1, (place == 0).astype(jnp.int32)]).astype(jnp.int32)

        sent = pl.pallas_call(
            pack_kernel,
            out_shape=jax.ShapeDtypeStruct(
                (2 * chips, row_steps, features + 2 * new_keys.shape[3]), jnp.bfloat16
            ),
            in_specs=[VMEM] * 3,
            out_specs=VMEM,
            compiler_params=limit(4),
            name="pack",
        )(queries[0], new_keys[0], new_values[0])
        own = exchange(sent, same_core)
        other = lax.ppermute(own, "tp", across)

        block_rows = half_rs * local_heads + 2 * half_rs
        state = jax.ShapeDtypeStruct((2, chips, block_rows, HD), jnp.bfloat16)
        keep, send = pl.pallas_call(
            lambda *refs: attend_kernel(chips, *refs),
            out_shape=(state, state),
            in_specs=[SMEM, SMEM] + [VMEM] * 6,
            out_specs=(VMEM, VMEM),
            scratch_shapes=[
                pltpu.VMEM((row_steps, tokens), jnp.float32),
                pltpu.VMEM((GS * steps, tokens), jnp.float32),
            ],
            compiler_params=limit(16),
            name="attend",
        )(
            info,
            target_slot[0],
            page_owner,
            page_fill,
            own,
            other,
            key_pages.reshape(tokens, key_pages.shape[3]),
            value_pages.reshape(tokens, value_pages.shape[3]),
        )
        merged = pl.pallas_call(
            lambda *refs: merge_kernel(local_heads, *refs),
            out_shape=state,
            in_specs=[VMEM, VMEM],
            out_specs=VMEM,
            compiler_params=limit(4),
            name="merge",
        )(keep, lax.ppermute(send, "tp", across))
        arrived = exchange(merged.reshape(2 * chips, block_rows, HD), same_core)
        finished = pl.pallas_call(
            lambda *refs: reduce_kernel(chips, steps, *refs),
            out_shape=jax.ShapeDtypeStruct((2, chips, half_rs, features), jnp.bfloat16),
            in_specs=[SMEM, VMEM],
            out_specs=VMEM,
            compiler_params=limit(4),
            name="reduce",
        )(info, arrived)
        own = exchange(finished.reshape(2 * chips, half_rs, features), same_core)
        other = lax.ppermute(own, "tp", across)
        projected = pl.pallas_call(
            lambda *refs: project_kernel(chips, *refs),
            out_shape=jax.ShapeDtypeStruct((rows, steps, out_weight.shape[1]), jnp.bfloat16),
            in_specs=[SMEM, VMEM, VMEM, VMEM],
            out_specs=VMEM,
            compiler_params=limit(16),
            name="project",
        )(info, own, other, out_weight.reshape(width, features, out_weight.shape[1]))
        return projected[None]

    return per_device


def solution(mesh):
    placed = (
        P("group", None, None, "tp"),
        P("group", None, None, "tp"),
        P("group", None, None, "tp"),
        P("group", "tp", None, None),
        P("group", "tp", None, None),
        P("group", "tp"),
        P("group", "tp"),
        P("group", None),
        P(None, "tp"),
    )
    return jax.shard_map(
        per_device_of(mesh.shape["group"], mesh.shape["tp"]),
        mesh=mesh,
        in_specs=placed,
        out_specs=P("group", None, None, "tp"),
        check_vma=False,
    )
```

```python
import math

import jax
import jax.numpy as jnp
from jax import lax
from jax.experimental import pallas as pl
from jax.experimental.pallas import tpu as pltpu
from jax.sharding import PartitionSpec as P

HEADS = 64
KVH = 8
HD = 128
PAGE = 16
NEG = -1e30
FLOOR = -1e29
SCALE = 1.0 / math.sqrt(HD) * math.log2(math.e)
MOVED_LANE = 64
TARGET_LANE = 127
GS = HEADS // KVH
UNROLL = 1


def dot(a, b, contract):
    return lax.dot_general(a, b, ((contract), ((), ())), preferred_element_type=jnp.float32)


def iota(shape, axis):
    return lax.broadcasted_iota(jnp.int32, shape, axis)


def pack_kernel(queries, new_keys, new_values, out, q_buf, k_buf, v_buf, sems):
    row_steps = out.shape[1]
    buffers = (q_buf, k_buf, v_buf)
    copies = [
        pltpu.make_async_copy(x, b, sems.at[i])
        for i, (x, b) in enumerate(zip((queries, new_keys, new_values), buffers))
    ]
    for c in copies:
        c.start()
    for c in copies:
        c.wait()
    row = jnp.concatenate([b[...].reshape(row_steps, b.shape[2]) for b in buffers], axis=1)
    for i in range(out.shape[0]):
        out[i] = row


def sums_of(aux, local_heads):
    high = pltpu.roll(aux, HD - local_heads, 1)
    return high + pltpu.roll(aux, HD - 2 * local_heads, 1)


def split(total):
    high = total.astype(jnp.bfloat16).astype(jnp.float32)
    return high, total - high


def attend_kernel(
    chips,
    info,
    slots_hbm,
    owner_hbm,
    fill_hbm,
    own,
    other,
    keys_hbm,
    values_hbm,
    weight_hbm,
    keep,
    send,
    weight,
    bias_own,
    bias_moved,
    slots,
    owner,
    fill,
    keys,
    values,
    small_sems,
    kv_sems,
    weight_sems,
):
    row_steps = own.shape[1]
    rows = slots.shape[1]
    steps = row_steps // rows
    features = HEADS // (2 * chips) * HD
    local_heads = features // HD
    kv_part = (own.shape[2] - features) // 2
    per_kv = chips // KVH
    tokens = keys.shape[1]
    half_rs = row_steps // 2
    pieces = weight.shape[0] // KVH

    def kv_copy(g, which):
        at = pl.ds(pl.multiple_of(g * HD, HD), HD)
        source, target = ((keys_hbm, keys), (values_hbm, values))[which]
        return pltpu.make_async_copy(source.at[:, at], target.at[g], kv_sems.at[which, g])

    def weight_copy(g):
        at = pl.ds(g * pieces, pieces)
        return pltpu.make_async_copy(weight_hbm.at[at], weight.at[at], weight_sems.at[g])

    small = [
        pltpu.make_async_copy(source, target, small_sems.at[i])
        for i, (source, target) in enumerate(
            ((slots_hbm, slots), (owner_hbm, owner), (fill_hbm, fill))
        )
    ]
    for c in small:
        c.start()
    for g in range(KVH):
        kv_copy(g, 0).start()
        kv_copy(g, 1).start()
    for c in small:
        c.wait()
    half = info[0]
    core = info[1]
    first = info[2]
    mover = jnp.int32(0)
    target = jnp.int32(0)
    for r in range(rows):
        leaves = slots[0, r] < rows
        mover = jnp.where(leaves, r, mover)
        target = jnp.where(leaves, slots[0, r], target)

    pages = owner.shape[1]
    spread = (iota((pages, tokens), 1) // PAGE == iota((pages, tokens), 0)).astype(jnp.bfloat16)
    table = jnp.concatenate([owner[...], fill[...]], axis=0).astype(jnp.float32)
    table = jnp.concatenate([table] * 4, axis=0).astype(jnp.bfloat16)
    by_token = dot(table, spread, ((1,), (0,)))
    owner_tok = by_token[0:1].astype(jnp.int32)
    fill_tok = by_token[1:2].astype(jnp.int32)
    live = iota((1, tokens), 1) % PAGE < fill_tok
    token_row = jnp.where(live, owner_tok, rows)
    stay_row = jnp.where(token_row == mover, rows, token_row)
    bias_own[...] = jnp.where(iota((row_steps, tokens), 0) // steps == stay_row, 0.0, NEG)
    bias_moved[...] = jnp.broadcast_to(jnp.where(token_row == mover, 0.0, NEG), bias_moved.shape)

    rs_ids = iota((row_steps, row_steps), 0)
    new_ids = iota((row_steps, row_steps), 1)
    new_live = (rs_ids // steps == new_ids // steps) & (new_ids % steps <= rs_ids % steps)
    bias_new = jnp.where(new_live & (first == 1), 0.0, NEG)
    moved_rows = GS * steps
    wide = GS * row_steps
    pick_ids = iota((moved_rows, wide), 0)
    pick = (
        iota((moved_rows, wide), 1)
        == (pick_ids // steps) * row_steps + target * steps + pick_ids % steps
    ).astype(jnp.bfloat16)
    lane = iota((half_rs, HD), 1)
    target_f = target.astype(jnp.float32)

    def per_head(g, carry):
        weight_copy(g).start()
        kv_copy(g, 0).wait()
        kv_copy(g, 1).wait()
        tiles, partner_tiles, new_k, new_v = [], [], [], []
        for source in (own, other):
            for kl in range(per_kv):
                mine = source[half * chips + g * per_kv + kl]
                theirs = source[(1 - half) * chips + g * per_kv + kl]
                for j in range(local_heads):
                    tiles.append(mine[:, j * HD : (j + 1) * HD])
                    partner_tiles.append(theirs[:, j * HD : (j + 1) * HD])
                new_k.append(mine[:, features : features + kv_part])
                new_v.append(mine[:, features + kv_part :])

        def in_order(parts):
            mine, theirs = parts[:per_kv], parts[per_kv:]
            a = [x for pair in zip(mine, theirs) for x in pair]
            b = [x for pair in zip(theirs, mine) for x in pair]
            return jnp.where(
                core == 0,
                jnp.concatenate(a, axis=1).astype(jnp.float32),
                jnp.concatenate(b, axis=1).astype(jnp.float32),
            ).astype(jnp.bfloat16)

        moved_q = dot(pick, jnp.concatenate(partner_tiles, axis=0), ((1,), (0,)))
        q = jnp.concatenate(tiles + [moved_q.astype(jnp.bfloat16)], axis=0)
        k = keys[g]
        v = values[g]
        scores = dot(q, k, ((1,), (1,))) * SCALE
        bias = jnp.concatenate([bias_own[...]] * GS + [bias_moved[...]], axis=0)
        scores = scores + bias
        new_scores = dot(q[:wide], in_order(new_k), ((1,), (1,))) * SCALE
        new_scores = new_scores + jnp.concatenate([bias_new] * GS, axis=0)
        new_scores = jnp.concatenate(
            [new_scores, jnp.full((moved_rows, row_steps), NEG, jnp.float32)], axis=0
        )
        top = jnp.maximum(
            jnp.max(scores, axis=1, keepdims=True), jnp.max(new_scores, axis=1, keepdims=True)
        )
        top = jnp.maximum(top, FLOOR).astype(jnp.bfloat16).astype(jnp.float32)
        p = jnp.exp2(scores - top).astype(jnp.bfloat16)
        pn = jnp.exp2(new_scores - top).astype(jnp.bfloat16)
        total = jnp.sum(p.astype(jnp.float32), axis=1, keepdims=True) + jnp.sum(
            pn.astype(jnp.float32), axis=1, keepdims=True
        )
        acc = dot(p, v, ((1,), (0,))) + dot(pn, in_order(new_v), ((1,), (0,)))
        high, low = split(total)

        for side in range(2):
            for kl in range(per_kv):
                t0 = (side * per_kv + kl) * local_heads
                at_moved = slice(wide + t0 * steps, wide + (t0 + local_heads) * steps)
                moved_acc = acc[at_moved]
                short = half_rs - local_heads * steps

                def filled(x):
                    if short == 0:
                        return x
                    return jnp.concatenate([x, jnp.zeros((short, x.shape[1]), x.dtype)], axis=0)

                for h in range(2):
                    parts = [
                        acc[(t0 + j) * row_steps + h * half_rs :][:half_rs]
                        for j in range(local_heads)
                    ]
                    aux = jnp.where(lane == MOVED_LANE, filled(top[at_moved]), 0.0)
                    aux = jnp.where(lane == MOVED_LANE + local_heads, filled(high[at_moved]), aux)
                    aux = jnp.where(lane == MOVED_LANE + 2 * local_heads, filled(low[at_moved]), aux)
                    aux = jnp.where(lane == TARGET_LANE, target_f, aux)
                    for j in range(local_heads):
                        rows_at = slice(
                            (t0 + j) * row_steps + h * half_rs,
                            (t0 + j) * row_steps + (h + 1) * half_rs,
                        )
                        aux = jnp.where(lane == j, top[rows_at], aux)
                        aux = jnp.where(lane == local_heads + j, high[rows_at], aux)
                        aux = jnp.where(lane == 2 * local_heads + j, low[rows_at], aux)
                    block = jnp.concatenate(parts + [filled(moved_acc), aux], axis=0)
                    dest = keep if side == 0 else send
                    dest[h, g * per_kv + kl] = block.astype(jnp.bfloat16)
        return carry

    lax.fori_loop(0, KVH, per_head, 0, unroll=UNROLL)
    for g in range(KVH):
        weight_copy(g).wait()


def merge_kernel(local_heads, first, second, out):
    half_rs = (first.shape[2]) // (local_heads + 2)
    span = half_rs * local_heads
    lane = iota((half_rs, HD), 1)
    for h in range(first.shape[0]):
        for k in range(first.shape[1]):
            a = first[h, k].astype(jnp.float32)
            b = second[h, k].astype(jnp.float32)
            aux_a, aux_b = a[span + half_rs :], b[span + half_rs :]
            top = jnp.maximum(aux_a, aux_b)
            wa = jnp.exp2(aux_a - top)
            wb = jnp.exp2(aux_b - top)
            total = wa * sums_of(aux_a, local_heads) + wb * sums_of(aux_b, local_heads)
            high, low = split(total)
            is_top = (lane < local_heads) | (lane >= MOVED_LANE)
            is_top = is_top & (lane < MOVED_LANE + local_heads) | (lane == TARGET_LANE)
            high = pltpu.roll(high, local_heads, 1)
            low = pltpu.roll(low, 2 * local_heads, 1)
            part = lane % MOVED_LANE // local_heads
            aux = jnp.where(is_top, top, jnp.where(part == 1, high, low))
            parts = []
            for j in range(local_heads + 1):
                at = j if j < local_heads else MOVED_LANE
                rows = slice(j * half_rs, (j + 1) * half_rs)
                parts.append(wa[:, at : at + 1] * a[rows] + wb[:, at : at + 1] * b[rows])
            out[h, k] = jnp.concatenate(parts + [aux], axis=0).astype(jnp.bfloat16)


def reduce_kernel(chips, steps, info, parts, out):
    half_rs = out.shape[2]
    local_heads = out.shape[3] // HD
    half = info[0]
    span = half_rs * local_heads
    row_ids = iota((half_rs, 1), 0)
    tops, sums, accs = [], [], []
    for g in range(2):
        aux = [
            parts[g * chips + k, span + half_rs :].astype(jnp.float32) for k in range(chips)
        ]
        top = aux[0]
        for a in aux[1:]:
            top = jnp.maximum(top, a)
        total = None
        acc = [None] * (local_heads + 1)
        for k in range(chips):
            w = jnp.exp2(aux[k] - top)
            part = w * sums_of(aux[k], local_heads)
            total = part if total is None else total + part
            for j in range(local_heads + 1):
                at = j if j < local_heads else MOVED_LANE
                block = parts[g * chips + k, j * half_rs : (j + 1) * half_rs]
                part = w[:, at : at + 1] * block.astype(jnp.float32)
                acc[j] = part if acc[j] is None else acc[j] + part
        tops.append(top)
        sums.append(total)
        accs.append(acc)
    for g in range(2):
        slot = tops[1 - g][:, TARGET_LANE : TARGET_LANE + 1]
        mine = (half_rs // steps * half + row_ids // steps).astype(jnp.float32) == slot
        moved_top = tops[1 - g][:, MOVED_LANE : MOVED_LANE + 1]
        moved_sum = sums[1 - g][:, MOVED_LANE : MOVED_LANE + 1]
        moved_acc = accs[1 - g][local_heads]
        done = []
        for j in range(local_heads):

            def placed(x):
                y = jnp.broadcast_to(x[j * steps : j * steps + 1], (half_rs, x.shape[1]))
                for s in range(1, steps):
                    z = jnp.broadcast_to(x[j * steps + s : j * steps + s + 1], y.shape)
                    y = jnp.where(row_ids % steps == s, z, y)
                return y

            own_top = tops[g][:, j : j + 1]
            in_top = jnp.where(mine, placed(moved_top), FLOOR)
            top = jnp.maximum(own_top, in_top)
            w_own = jnp.exp2(own_top - top)
            w_in = jnp.where(mine, jnp.exp2(in_top - top), 0.0)
            total = w_own * sums[g][:, j : j + 1] + w_in * placed(moved_sum)
            done.append((w_own * accs[g][j] + w_in * placed(moved_acc)) / total)
        result = jnp.concatenate(done, axis=1).astype(jnp.bfloat16)
        for k in range(chips):
            out[g, k] = result


def project_kernel(chips, info, own, other, weight, out):
    core = info[1]
    acc = None
    for side, source in enumerate((own, other)):
        which = core if side == 0 else 1 - core
        for k in range(chips):
            x = jnp.concatenate([source[k], source[chips + k]], axis=0)
            part = dot(x, weight[2 * k + which], ((1,), (0,)))
            acc = part if acc is None else acc + part
    out[...] = acc.astype(jnp.bfloat16).reshape(out.shape)


def in_hbm(x):
    return pltpu.with_memory_space_constraint(x, pltpu.HBM)


def limit(mib):
    return pltpu.CompilerParams(vmem_limit_bytes=mib << 20)


SMEM = pl.BlockSpec(memory_space=pltpu.SMEM)
VMEM = pl.BlockSpec(memory_space=pltpu.VMEM)
HBM = pl.BlockSpec(memory_space=pltpu.HBM)


def per_device_of(groups, width):
    chips = width // 2
    apart = groups // 2
    same_core = [
        [(g + h * apart) * width + 2 * k + c for h in range(2) for k in range(chips)]
        for g in range(apart)
        for c in range(2)
    ]
    across = [(t, t ^ 1) for t in range(width)]
    both = ("group", "tp")

    def exchange(x, members):
        return lax.all_to_all(x, both, 0, 0, axis_index_groups=members)

    def per_device(
        queries,
        new_keys,
        new_values,
        key_pages,
        value_pages,
        page_owner,
        page_fill,
        target_slot,
        out_weight,
    ):
        rows, steps, features = queries.shape[1:]
        local_heads = features // HD
        row_steps = rows * steps
        half_rs = row_steps // 2
        pages = key_pages.shape[1]
        tokens = pages * PAGE
        place = lax.axis_index("tp")
        half = lax.axis_index("group") // apart
        info = jnp.stack([half, place & 1, (place == 0).astype(jnp.int32)]).astype(jnp.int32)

        sent = pl.pallas_call(
            pack_kernel,
            out_shape=jax.ShapeDtypeStruct(
                (2 * chips, row_steps, features + 2 * new_keys.shape[3]), jnp.bfloat16
            ),
            in_specs=[HBM] * 3,
            out_specs=VMEM,
            scratch_shapes=[
                pltpu.VMEM(x.shape[1:], x.dtype) for x in (queries, new_keys, new_values)
            ]
            + [pltpu.SemaphoreType.DMA((3,))],
            compiler_params=limit(4),
            name="pack",
        )(*(in_hbm(x[0]) for x in (queries, new_keys, new_values)))
        own = exchange(sent, same_core)
        other = lax.ppermute(own, "tp", across)

        block_rows = half_rs * local_heads + 2 * half_rs
        state = jax.ShapeDtypeStruct((2, chips, block_rows, HD), jnp.bfloat16)
        weight_by_device = out_weight.reshape(width, features, out_weight.shape[1])
        keep, send, weight = pl.pallas_call(
            lambda *refs: attend_kernel(chips, *refs),
            out_shape=(
                state,
                state,
                jax.ShapeDtypeStruct(weight_by_device.shape, weight_by_device.dtype),
            ),
            in_specs=[SMEM] + [HBM] * 3 + [VMEM] * 2 + [HBM] * 3,
            out_specs=(VMEM, VMEM, VMEM),
            scratch_shapes=[
                pltpu.VMEM((row_steps, tokens), jnp.float32),
                pltpu.VMEM((GS * steps, tokens), jnp.float32),
                pltpu.SMEM(target_slot.shape, jnp.int32),
                pltpu.VMEM(page_owner.shape, jnp.int32),
                pltpu.VMEM(page_fill.shape, jnp.int32),
                pltpu.VMEM((KVH, tokens, HD), jnp.bfloat16),
                pltpu.VMEM((KVH, tokens, HD), jnp.bfloat16),
                pltpu.SemaphoreType.DMA((3,)),
                pltpu.SemaphoreType.DMA((2, KVH)),
                pltpu.SemaphoreType.DMA((KVH,)),
            ],
            compiler_params=limit(28),
            name="attend",
        )(
            info,
            in_hbm(target_slot),
            in_hbm(page_owner),
            in_hbm(page_fill),
            own,
            other,
            in_hbm(key_pages.reshape(tokens, key_pages.shape[3])),
            in_hbm(value_pages.reshape(tokens, value_pages.shape[3])),
            in_hbm(weight_by_device),
        )
        merged = pl.pallas_call(
            lambda *refs: merge_kernel(local_heads, *refs),
            out_shape=state,
            in_specs=[VMEM, VMEM],
            out_specs=VMEM,
            compiler_params=limit(4),
            name="merge",
        )(keep, lax.ppermute(send, "tp", across))
        arrived = exchange(merged.reshape(2 * chips, block_rows, HD), same_core)
        finished = pl.pallas_call(
            lambda *refs: reduce_kernel(chips, steps, *refs),
            out_shape=jax.ShapeDtypeStruct((2, chips, half_rs, features), jnp.bfloat16),
            in_specs=[SMEM, VMEM],
            out_specs=VMEM,
            compiler_params=limit(4),
            name="reduce",
        )(info, arrived)
        own = exchange(finished.reshape(2 * chips, half_rs, features), same_core)
        other = lax.ppermute(own, "tp", across)
        projected = pl.pallas_call(
            lambda *refs: project_kernel(chips, *refs),
            out_shape=jax.ShapeDtypeStruct((rows, steps, out_weight.shape[1]), jnp.bfloat16),
            in_specs=[SMEM, VMEM, VMEM, VMEM],
            out_specs=VMEM,
            compiler_params=limit(16),
            name="project",
        )(info, own, other, weight)
        return projected[None]

    return per_device


def solution(mesh):
    placed = (
        P("group", None, None, "tp"),
        P("group", None, None, "tp"),
        P("group", None, None, "tp"),
        P("group", "tp", None, None),
        P("group", "tp", None, None),
        P("group", "tp"),
        P("group", "tp"),
        P("group", None),
        P(None, "tp"),
    )
    return jax.shard_map(
        per_device_of(mesh.shape["group"], mesh.shape["tp"]),
        mesh=mesh,
        in_specs=placed,
        out_specs=P("group", None, None, "tp"),
        check_vma=False,
    )
```

```python
import math

import jax
import jax.numpy as jnp
from jax import lax
from jax.experimental import pallas as pl
from jax.experimental.pallas import tpu as pltpu
from jax.sharding import PartitionSpec as P

HEADS = 64
KVH = 8
HD = 128
PAGE = 16
NEG = -1e30
FLOOR = -1e29
SCALE = 1.0 / math.sqrt(HD) * math.log2(math.e)
MOVED_LANE = 64
TARGET_LANE = 127
GS = HEADS // KVH
UNROLL = 2


def dot(a, b, contract):
    return lax.dot_general(a, b, ((contract), ((), ())), preferred_element_type=jnp.float32)


def iota(shape, axis):
    return lax.broadcasted_iota(jnp.int32, shape, axis)


def pack_kernel(queries, new_keys, new_values, out, q_buf, k_buf, v_buf, sems):
    row_steps = out.shape[1]
    buffers = (q_buf, k_buf, v_buf)
    copies = [
        pltpu.make_async_copy(x, b, sems.at[i])
        for i, (x, b) in enumerate(zip((queries, new_keys, new_values), buffers))
    ]
    for c in copies:
        c.start()
    for c in copies:
        c.wait()
    row = jnp.concatenate([b[...].reshape(row_steps, b.shape[2]) for b in buffers], axis=1)
    for i in range(out.shape[0]):
        out[i] = row


def sums_of(aux, local_heads):
    high = pltpu.roll(aux, HD - local_heads, 1)
    return high + pltpu.roll(aux, HD - 2 * local_heads, 1)


def split(total):
    high = total.astype(jnp.bfloat16).astype(jnp.float32)
    return high, total - high


def mover_of(slots):
    rows = slots.shape[1]
    mover = jnp.int32(0)
    target = jnp.int32(0)
    for r in range(rows):
        leaves = slots[0, r] < rows
        mover = jnp.where(leaves, r, mover)
        target = jnp.where(leaves, slots[0, r], target)
    return mover, target


def prepare_kernel(
    steps,
    slots_hbm,
    owner_hbm,
    fill_hbm,
    keys_hbm,
    values_hbm,
    after,
    keys,
    values,
    bias_own,
    bias_moved,
    slots,
    owner,
    fill,
    sems,
):
    del after
    rows = slots.shape[1]
    row_steps, tokens = bias_own.shape
    sources = (slots_hbm, owner_hbm, fill_hbm, keys_hbm, values_hbm)
    targets = (slots, owner, fill, keys, values)
    copies = [
        pltpu.make_async_copy(source, target, sems.at[i])
        for i, (source, target) in enumerate(zip(sources, targets))
    ]
    for c in copies:
        c.start()
    for c in copies[:3]:
        c.wait()
    mover, _ = mover_of(slots)
    pages = owner.shape[1]
    spread = (iota((pages, tokens), 1) // PAGE == iota((pages, tokens), 0)).astype(jnp.bfloat16)
    table = jnp.concatenate([owner[...], fill[...]], axis=0).astype(jnp.float32)
    table = jnp.concatenate([table] * 4, axis=0).astype(jnp.bfloat16)
    by_token = dot(table, spread, ((1,), (0,)))
    owner_tok = by_token[0:1].astype(jnp.int32)
    fill_tok = by_token[1:2].astype(jnp.int32)
    live = iota((1, tokens), 1) % PAGE < fill_tok
    token_row = jnp.where(live, owner_tok, rows)
    stay_row = jnp.where(token_row == mover, rows, token_row)
    bias_own[...] = jnp.where(iota((row_steps, tokens), 0) // steps == stay_row, 0.0, NEG)
    bias_moved[...] = jnp.broadcast_to(jnp.where(token_row == mover, 0.0, NEG), bias_moved.shape)
    for c in copies[3:]:
        c.wait()


def attend_kernel(
    chips,
    info,
    slots,
    own,
    other,
    keys,
    values,
    bias_own,
    bias_moved,
    weight_hbm,
    keep,
    send,
    weight,
    weight_sems,
):
    row_steps = own.shape[1]
    steps = row_steps // slots.shape[1]
    features = HEADS // (2 * chips) * HD
    local_heads = features // HD
    kv_part = (own.shape[2] - features) // 2
    per_kv = chips // KVH
    half_rs = row_steps // 2
    half = info[0]
    core = info[1]
    first = info[2]
    _, target = mover_of(slots)
    copies = [
        pltpu.make_async_copy(weight_hbm.at[i], weight.at[i], weight_sems.at[i])
        for i in range(weight.shape[0])
    ]
    for c in copies:
        c.start()

    rs_ids = iota((row_steps, row_steps), 0)
    new_ids = iota((row_steps, row_steps), 1)
    new_live = (rs_ids // steps == new_ids // steps) & (new_ids % steps <= rs_ids % steps)
    bias_new = jnp.where(new_live & (first == 1), 0.0, NEG)
    moved_rows = GS * steps
    wide = GS * row_steps
    pick_ids = iota((moved_rows, wide), 0)
    pick = (
        iota((moved_rows, wide), 1)
        == (pick_ids // steps) * row_steps + target * steps + pick_ids % steps
    ).astype(jnp.bfloat16)
    lane = iota((half_rs, HD), 1)
    target_f = target.astype(jnp.float32)

    def per_head(g, carry):
        tiles, partner_tiles, new_k, new_v = [], [], [], []
        for source in (own, other):
            for kl in range(per_kv):
                mine = source[half * chips + g * per_kv + kl]
                theirs = source[(1 - half) * chips + g * per_kv + kl]
                for j in range(local_heads):
                    tiles.append(mine[:, j * HD : (j + 1) * HD])
                    partner_tiles.append(theirs[:, j * HD : (j + 1) * HD])
                new_k.append(mine[:, features : features + kv_part])
                new_v.append(mine[:, features + kv_part :])

        def in_order(parts):
            mine, theirs = parts[:per_kv], parts[per_kv:]
            a = [x for pair in zip(mine, theirs) for x in pair]
            b = [x for pair in zip(theirs, mine) for x in pair]
            return jnp.where(
                core == 0,
                jnp.concatenate(a, axis=1).astype(jnp.float32),
                jnp.concatenate(b, axis=1).astype(jnp.float32),
            ).astype(jnp.bfloat16)

        moved_q = dot(pick, jnp.concatenate(partner_tiles, axis=0), ((1,), (0,)))
        q = jnp.concatenate(tiles + [moved_q.astype(jnp.bfloat16)], axis=0)
        at = pl.ds(pl.multiple_of(g * HD, HD), HD)
        k = keys[:, at]
        v = values[:, at]
        scores = dot(q, k, ((1,), (1,))) * SCALE
        bias = jnp.concatenate([bias_own[...]] * GS + [bias_moved[...]], axis=0)
        scores = scores + bias
        new_scores = dot(q[:wide], in_order(new_k), ((1,), (1,))) * SCALE
        new_scores = new_scores + jnp.concatenate([bias_new] * GS, axis=0)
        new_scores = jnp.concatenate(
            [new_scores, jnp.full((moved_rows, row_steps), NEG, jnp.float32)], axis=0
        )
        top = jnp.maximum(
            jnp.max(scores, axis=1, keepdims=True), jnp.max(new_scores, axis=1, keepdims=True)
        )
        top = jnp.maximum(top, FLOOR).astype(jnp.bfloat16).astype(jnp.float32)
        p = jnp.exp2(scores - top).astype(jnp.bfloat16)
        pn = jnp.exp2(new_scores - top).astype(jnp.bfloat16)
        total = jnp.sum(p.astype(jnp.float32), axis=1, keepdims=True) + jnp.sum(
            pn.astype(jnp.float32), axis=1, keepdims=True
        )
        acc = dot(p, v, ((1,), (0,))) + dot(pn, in_order(new_v), ((1,), (0,)))
        high, low = split(total)

        for side in range(2):
            for kl in range(per_kv):
                t0 = (side * per_kv + kl) * local_heads
                at_moved = slice(wide + t0 * steps, wide + (t0 + local_heads) * steps)
                moved_acc = acc[at_moved]
                short = half_rs - local_heads * steps

                def filled(x):
                    if short == 0:
                        return x
                    return jnp.concatenate([x, jnp.zeros((short, x.shape[1]), x.dtype)], axis=0)

                for h in range(2):
                    parts = [
                        acc[(t0 + j) * row_steps + h * half_rs :][:half_rs]
                        for j in range(local_heads)
                    ]
                    aux = jnp.where(lane == MOVED_LANE, filled(top[at_moved]), 0.0)
                    aux = jnp.where(lane == MOVED_LANE + local_heads, filled(high[at_moved]), aux)
                    aux = jnp.where(lane == MOVED_LANE + 2 * local_heads, filled(low[at_moved]), aux)
                    aux = jnp.where(lane == TARGET_LANE, target_f, aux)
                    for j in range(local_heads):
                        rows_at = slice(
                            (t0 + j) * row_steps + h * half_rs,
                            (t0 + j) * row_steps + (h + 1) * half_rs,
                        )
                        aux = jnp.where(lane == j, top[rows_at], aux)
                        aux = jnp.where(lane == local_heads + j, high[rows_at], aux)
                        aux = jnp.where(lane == 2 * local_heads + j, low[rows_at], aux)
                    block = jnp.concatenate(parts + [filled(moved_acc), aux], axis=0)
                    dest = keep if side == 0 else send
                    dest[h, g * per_kv + kl] = block.astype(jnp.bfloat16)
        return carry

    lax.fori_loop(0, KVH, per_head, 0, unroll=UNROLL)
    for c in copies:
        c.wait()


def merge_kernel(local_heads, first, second, out):
    half_rs = (first.shape[2]) // (local_heads + 2)
    span = half_rs * local_heads
    lane = iota((half_rs, HD), 1)
    for h in range(first.shape[0]):
        for k in range(first.shape[1]):
            a = first[h, k].astype(jnp.float32)
            b = second[h, k].astype(jnp.float32)
            aux_a, aux_b = a[span + half_rs :], b[span + half_rs :]
            top = jnp.maximum(aux_a, aux_b)
            wa = jnp.exp2(aux_a - top)
            wb = jnp.exp2(aux_b - top)
            total = wa * sums_of(aux_a, local_heads) + wb * sums_of(aux_b, local_heads)
            high, low = split(total)
            is_top = (lane < local_heads) | (lane >= MOVED_LANE)
            is_top = is_top & (lane < MOVED_LANE + local_heads) | (lane == TARGET_LANE)
            high = pltpu.roll(high, local_heads, 1)
            low = pltpu.roll(low, 2 * local_heads, 1)
            part = lane % MOVED_LANE // local_heads
            aux = jnp.where(is_top, top, jnp.where(part == 1, high, low))
            parts = []
            for j in range(local_heads + 1):
                at = j if j < local_heads else MOVED_LANE
                rows = slice(j * half_rs, (j + 1) * half_rs)
                parts.append(wa[:, at : at + 1] * a[rows] + wb[:, at : at + 1] * b[rows])
            out[h, k] = jnp.concatenate(parts + [aux], axis=0).astype(jnp.bfloat16)


def reduce_kernel(chips, steps, info, parts, out):
    half_rs = out.shape[2]
    local_heads = out.shape[3] // HD
    half = info[0]
    span = half_rs * local_heads
    row_ids = iota((half_rs, 1), 0)
    tops, sums, accs = [], [], []
    for g in range(2):
        aux = [
            parts[g * chips + k, span + half_rs :].astype(jnp.float32) for k in range(chips)
        ]
        top = aux[0]
        for a in aux[1:]:
            top = jnp.maximum(top, a)
        total = None
        acc = [None] * (local_heads + 1)
        for k in range(chips):
            w = jnp.exp2(aux[k] - top)
            part = w * sums_of(aux[k], local_heads)
            total = part if total is None else total + part
            for j in range(local_heads + 1):
                at = j if j < local_heads else MOVED_LANE
                block = parts[g * chips + k, j * half_rs : (j + 1) * half_rs]
                part = w[:, at : at + 1] * block.astype(jnp.float32)
                acc[j] = part if acc[j] is None else acc[j] + part
        tops.append(top)
        sums.append(total)
        accs.append(acc)
    for g in range(2):
        slot = tops[1 - g][:, TARGET_LANE : TARGET_LANE + 1]
        mine = (half_rs // steps * half + row_ids // steps).astype(jnp.float32) == slot
        moved_top = tops[1 - g][:, MOVED_LANE : MOVED_LANE + 1]
        moved_sum = sums[1 - g][:, MOVED_LANE : MOVED_LANE + 1]
        moved_acc = accs[1 - g][local_heads]
        done = []
        for j in range(local_heads):

            def placed(x):
                y = jnp.broadcast_to(x[j * steps : j * steps + 1], (half_rs, x.shape[1]))
                for s in range(1, steps):
                    z = jnp.broadcast_to(x[j * steps + s : j * steps + s + 1], y.shape)
                    y = jnp.where(row_ids % steps == s, z, y)
                return y

            own_top = tops[g][:, j : j + 1]
            in_top = jnp.where(mine, placed(moved_top), FLOOR)
            top = jnp.maximum(own_top, in_top)
            w_own = jnp.exp2(own_top - top)
            w_in = jnp.where(mine, jnp.exp2(in_top - top), 0.0)
            total = w_own * sums[g][:, j : j + 1] + w_in * placed(moved_sum)
            done.append((w_own * accs[g][j] + w_in * placed(moved_acc)) / total)
        result = jnp.concatenate(done, axis=1).astype(jnp.bfloat16)
        for k in range(chips):
            out[g, k] = result


def project(chips, which, source, weight):
    acc = None
    for k in range(chips):
        x = jnp.concatenate([source[k], source[chips + k]], axis=0)
        part = dot(x, weight[2 * k + which], ((1,), (0,)))
        acc = part if acc is None else acc + part
    return acc


def project_own_kernel(chips, info, own, weight, out):
    out[...] = project(chips, info[1], own, weight)


def project_other_kernel(chips, info, partial, other, weight, out):
    total = partial[...] + project(chips, 1 - info[1], other, weight)
    out[...] = total.astype(jnp.bfloat16).reshape(out.shape)


def in_hbm(x):
    return pltpu.with_memory_space_constraint(x, pltpu.HBM)


def limit(mib):
    return pltpu.CompilerParams(vmem_limit_bytes=mib << 20)


SMEM = pl.BlockSpec(memory_space=pltpu.SMEM)
VMEM = pl.BlockSpec(memory_space=pltpu.VMEM)
HBM = pl.BlockSpec(memory_space=pltpu.HBM)
ANY = pl.BlockSpec(memory_space=pl.ANY)


def per_device_of(groups, width):
    chips = width // 2
    apart = groups // 2
    same_core = [
        [(g + h * apart) * width + 2 * k + c for h in range(2) for k in range(chips)]
        for g in range(apart)
        for c in range(2)
    ]
    across = [(t, t ^ 1) for t in range(width)]
    both = ("group", "tp")

    def exchange(x, members):
        return lax.all_to_all(x, both, 0, 0, axis_index_groups=members)

    def per_device(
        queries,
        new_keys,
        new_values,
        key_pages,
        value_pages,
        page_owner,
        page_fill,
        target_slot,
        out_weight,
    ):
        rows, steps, features = queries.shape[1:]
        local_heads = features // HD
        row_steps = rows * steps
        half_rs = row_steps // 2
        pages = key_pages.shape[1]
        tokens = pages * PAGE
        place = lax.axis_index("tp")
        half = lax.axis_index("group") // apart
        info = jnp.stack([half, place & 1, (place == 0).astype(jnp.int32)]).astype(jnp.int32)

        sent = pl.pallas_call(
            pack_kernel,
            out_shape=jax.ShapeDtypeStruct(
                (2 * chips, row_steps, features + 2 * new_keys.shape[3]), jnp.bfloat16
            ),
            in_specs=[HBM] * 3,
            out_specs=VMEM,
            scratch_shapes=[
                pltpu.VMEM(x.shape[1:], x.dtype) for x in (queries, new_keys, new_values)
            ]
            + [pltpu.SemaphoreType.DMA((3,))],
            compiler_params=limit(4),
            name="pack",
        )(*(in_hbm(x[0]) for x in (queries, new_keys, new_values)))
        own = exchange(sent, same_core)
        other = lax.ppermute(own, "tp", across)

        block_rows = half_rs * local_heads + 2 * half_rs
        state = jax.ShapeDtypeStruct((2, chips, block_rows, HD), jnp.bfloat16)
        ints = (target_slot, page_owner, page_fill)
        pages_shape = (tokens, key_pages.shape[3])
        keys, values, bias_own, bias_moved = pl.pallas_call(
            lambda *refs: prepare_kernel(steps, *refs),
            out_shape=(
                jax.ShapeDtypeStruct(pages_shape, key_pages.dtype),
                jax.ShapeDtypeStruct(pages_shape, value_pages.dtype),
                jax.ShapeDtypeStruct((row_steps, tokens), jnp.float32),
                jax.ShapeDtypeStruct((GS * steps, tokens), jnp.float32),
            ),
            in_specs=[HBM] * 5 + [ANY],
            out_specs=(VMEM,) * 4,
            scratch_shapes=[
                pltpu.SMEM(target_slot.shape, jnp.int32),
                pltpu.VMEM(page_owner.shape, jnp.int32),
                pltpu.VMEM(page_fill.shape, jnp.int32),
                pltpu.SemaphoreType.DMA((5,)),
            ],
            compiler_params=limit(8),
            name="prepare",
        )(
            *(in_hbm(x) for x in ints),
            in_hbm(key_pages.reshape(pages_shape)),
            in_hbm(value_pages.reshape(pages_shape)),
            own,
        )
        weight_by_device = out_weight.reshape(width, features, out_weight.shape[1])
        keep, send, weight = pl.pallas_call(
            lambda *refs: attend_kernel(chips, *refs),
            out_shape=(
                state,
                state,
                jax.ShapeDtypeStruct(weight_by_device.shape, weight_by_device.dtype),
            ),
            in_specs=[SMEM, SMEM] + [VMEM] * 6 + [HBM],
            out_specs=(VMEM, VMEM, VMEM),
            scratch_shapes=[pltpu.SemaphoreType.DMA((width,))],
            compiler_params=limit(24),
            name="attend",
        )(
            info,
            target_slot,
            own,
            other,
            keys,
            values,
            bias_own,
            bias_moved,
            in_hbm(weight_by_device),
        )
        merged = pl.pallas_call(
            lambda *refs: merge_kernel(local_heads, *refs),
            out_shape=state,
            in_specs=[VMEM, VMEM],
            out_specs=VMEM,
            compiler_params=limit(4),
            name="merge",
        )(keep, lax.ppermute(send, "tp", across))
        arrived = exchange(merged.reshape(2 * chips, block_rows, HD), same_core)
        finished = pl.pallas_call(
            lambda *refs: reduce_kernel(chips, steps, *refs),
            out_shape=jax.ShapeDtypeStruct((2, chips, half_rs, features), jnp.bfloat16),
            in_specs=[SMEM, VMEM],
            out_specs=VMEM,
            compiler_params=limit(4),
            name="reduce",
        )(info, arrived)
        own = exchange(finished.reshape(2 * chips, half_rs, features), same_core)
        other = lax.ppermute(own, "tp", across)
        partial = pl.pallas_call(
            lambda *refs: project_own_kernel(chips, *refs),
            out_shape=jax.ShapeDtypeStruct((row_steps, out_weight.shape[1]), jnp.float32),
            in_specs=[SMEM, VMEM, VMEM],
            out_specs=VMEM,
            compiler_params=limit(16),
            name="project_own",
        )(info, own, weight)
        projected = pl.pallas_call(
            lambda *refs: project_other_kernel(chips, *refs),
            out_shape=jax.ShapeDtypeStruct((rows, steps, out_weight.shape[1]), jnp.bfloat16),
            in_specs=[SMEM, VMEM, VMEM, VMEM],
            out_specs=VMEM,
            compiler_params=limit(16),
            name="project_other",
        )(info, partial, other, weight)
        return projected[None]

    return per_device


def solution(mesh):
    placed = (
        P("group", None, None, "tp"),
        P("group", None, None, "tp"),
        P("group", None, None, "tp"),
        P("group", "tp", None, None),
        P("group", "tp", None, None),
        P("group", "tp"),
        P("group", "tp"),
        P("group", None),
        P(None, "tp"),
    )
    return jax.shard_map(
        per_device_of(mesh.shape["group"], mesh.shape["tp"]),
        mesh=mesh,
        in_specs=placed,
        out_specs=P("group", None, None, "tp"),
        check_vma=False,
    )
```

```python
import math

import jax
import jax.numpy as jnp
from jax import lax
from jax.experimental import pallas as pl
from jax.experimental.pallas import tpu as pltpu
from jax.sharding import PartitionSpec as P

HEADS = 64
KVH = 8
HD = 128
PAGE = 16
NEG = -1e30
FLOOR = -1e29
SCALE = 1.0 / math.sqrt(HD) * math.log2(math.e)
MOVED_LANE = 64
TARGET_LANE = 127
GS = HEADS // KVH
UNROLL = 4


def dot(a, b, contract):
    return lax.dot_general(a, b, ((contract), ((), ())), preferred_element_type=jnp.float32)


def iota(shape, axis):
    return lax.broadcasted_iota(jnp.int32, shape, axis)


def pack_kernel(queries, new_keys, new_values, out, new_out, q_buf, k_buf, v_buf, sems):
    row_steps = out.shape[1]
    buffers = (q_buf, k_buf, v_buf)
    copies = [
        pltpu.make_async_copy(x, b, sems.at[i])
        for i, (x, b) in enumerate(zip((queries, new_keys, new_values), buffers))
    ]
    for c in copies:
        c.start()
    for c in copies:
        c.wait()
    rows = [b[...].reshape(row_steps, b.shape[2]) for b in buffers]
    for i in range(out.shape[0]):
        out[i] = rows[0]
    new_out[...] = jnp.concatenate(rows[1:], axis=1)


def sums_of(aux, local_heads):
    high = pltpu.roll(aux, HD - local_heads, 1)
    return high + pltpu.roll(aux, HD - 2 * local_heads, 1)


def split(total):
    high = total.astype(jnp.bfloat16).astype(jnp.float32)
    return high, total - high


def mover_of(slots):
    rows = slots.shape[1]
    mover = jnp.int32(0)
    target = jnp.int32(0)
    for r in range(rows):
        leaves = slots[0, r] < rows
        mover = jnp.where(leaves, r, mover)
        target = jnp.where(leaves, slots[0, r], target)
    return mover, target


def prepare_kernel(
    steps,
    slots_hbm,
    owner_hbm,
    fill_hbm,
    keys_hbm,
    values_hbm,
    after,
    keys,
    values,
    bias_own,
    bias_moved,
    slots,
    owner,
    fill,
    sems,
):
    del after
    rows = slots.shape[1]
    row_steps, tokens = bias_own.shape
    sources = (slots_hbm, owner_hbm, fill_hbm, keys_hbm, values_hbm)
    targets = (slots, owner, fill, keys, values)
    copies = [
        pltpu.make_async_copy(source, target, sems.at[i])
        for i, (source, target) in enumerate(zip(sources, targets))
    ]
    for c in copies:
        c.start()
    for c in copies[:3]:
        c.wait()
    mover, _ = mover_of(slots)
    pages = owner.shape[1]
    spread = (iota((pages, tokens), 1) // PAGE == iota((pages, tokens), 0)).astype(jnp.bfloat16)
    table = jnp.concatenate([owner[...], fill[...]], axis=0).astype(jnp.float32)
    table = jnp.concatenate([table] * 4, axis=0).astype(jnp.bfloat16)
    by_token = dot(table, spread, ((1,), (0,)))
    owner_tok = by_token[0:1].astype(jnp.int32)
    fill_tok = by_token[1:2].astype(jnp.int32)
    live = iota((1, tokens), 1) % PAGE < fill_tok
    token_row = jnp.where(live, owner_tok, rows)
    stay_row = jnp.where(token_row == mover, rows, token_row)
    bias_own[...] = jnp.where(iota((row_steps, tokens), 0) // steps == stay_row, 0.0, NEG)
    bias_moved[...] = jnp.broadcast_to(jnp.where(token_row == mover, 0.0, NEG), bias_moved.shape)
    for c in copies[3:]:
        c.wait()


def attend_kernel(
    chips,
    info,
    slots,
    own,
    other,
    keys,
    values,
    bias_own,
    bias_moved,
    weight_hbm,
    *rest,
):
    *new_tokens, keep, send, weight, weight_sems = rest
    row_steps = own.shape[1]
    steps = row_steps // slots.shape[1]
    features = HEADS // (2 * chips) * HD
    local_heads = features // HD
    kv_part = new_tokens[0].shape[1] // 2
    per_kv = chips // KVH
    half_rs = row_steps // 2
    half = info[0]
    spot = info[2]
    own_kv = info[3]
    _, target = mover_of(slots)
    copies = [
        pltpu.make_async_copy(weight_hbm.at[i], weight.at[i], weight_sems.at[i])
        for i in range(weight.shape[0])
    ]
    for c in copies:
        c.start()

    rs_ids = iota((row_steps, row_steps), 0)
    new_ids = iota((row_steps, row_steps), 1)
    new_live = (rs_ids // steps == new_ids // steps) & (new_ids % steps <= rs_ids % steps)
    bias_new = jnp.where(new_live & (spot == 0), 0.0, NEG)
    pieces = []
    for p in range(len(new_tokens)):
        piece = new_tokens[0][...].astype(jnp.float32)
        for i in range(1, len(new_tokens)):
            piece = jnp.where(spot == p ^ i, new_tokens[i][...].astype(jnp.float32), piece)
        pieces.append(piece)
    new_k = jnp.concatenate([x[:, :kv_part] for x in pieces], axis=1).astype(jnp.bfloat16)
    new_v = jnp.concatenate([x[:, kv_part:] for x in pieces], axis=1).astype(jnp.bfloat16)
    moved_rows = GS * steps
    wide = GS * row_steps
    pick_ids = iota((moved_rows, wide), 0)
    pick = (
        iota((moved_rows, wide), 1)
        == (pick_ids // steps) * row_steps + target * steps + pick_ids % steps
    ).astype(jnp.bfloat16)
    lane = iota((half_rs, HD), 1)
    target_f = target.astype(jnp.float32)

    def per_head(g, carry):
        tiles, partner_tiles = [], []
        for source in (own, other):
            for kl in range(per_kv):
                mine = source[half * chips + g * per_kv + kl]
                theirs = source[(1 - half) * chips + g * per_kv + kl]
                for j in range(local_heads):
                    tiles.append(mine[:, j * HD : (j + 1) * HD])
                    partner_tiles.append(theirs[:, j * HD : (j + 1) * HD])
        moved_q = dot(pick, jnp.concatenate(partner_tiles, axis=0), ((1,), (0,)))
        q = jnp.concatenate(tiles + [moved_q.astype(jnp.bfloat16)], axis=0)
        at = pl.ds(pl.multiple_of(g * HD, HD), HD)
        k = keys[:, at]
        v = values[:, at]
        scores = dot(q, k, ((1,), (1,))) * SCALE
        bias = jnp.concatenate([bias_own[...]] * GS + [bias_moved[...]], axis=0)
        scores = scores + bias
        new_scores = dot(q[:wide], new_k, ((1,), (1,))) * SCALE
        bias = jnp.where(g == own_kv, bias_new, NEG)
        new_scores = new_scores + jnp.concatenate([bias] * GS, axis=0)
        new_scores = jnp.concatenate(
            [new_scores, jnp.full((moved_rows, row_steps), NEG, jnp.float32)], axis=0
        )
        top = jnp.maximum(
            jnp.max(scores, axis=1, keepdims=True), jnp.max(new_scores, axis=1, keepdims=True)
        )
        top = jnp.maximum(top, FLOOR).astype(jnp.bfloat16).astype(jnp.float32)
        p = jnp.exp2(scores - top).astype(jnp.bfloat16)
        pn = jnp.exp2(new_scores - top).astype(jnp.bfloat16)
        total = jnp.sum(p.astype(jnp.float32), axis=1, keepdims=True) + jnp.sum(
            pn.astype(jnp.float32), axis=1, keepdims=True
        )
        acc = dot(p, v, ((1,), (0,))) + dot(pn, new_v, ((1,), (0,)))
        top_part, low_part = split(total)

        for side in range(2):
            for kl in range(per_kv):
                t0 = (side * per_kv + kl) * local_heads
                at_moved = slice(wide + t0 * steps, wide + (t0 + local_heads) * steps)
                moved_acc = acc[at_moved]
                short = half_rs - local_heads * steps

                def filled(x):
                    if short == 0:
                        return x
                    return jnp.concatenate([x, jnp.zeros((short, x.shape[1]), x.dtype)], axis=0)

                for h in range(2):
                    parts = [
                        acc[(t0 + j) * row_steps + h * half_rs :][:half_rs]
                        for j in range(local_heads)
                    ]
                    aux = jnp.where(lane == MOVED_LANE, filled(top[at_moved]), 0.0)
                    aux = jnp.where(lane == MOVED_LANE + local_heads, filled(top_part[at_moved]), aux)
                    aux = jnp.where(lane == MOVED_LANE + 2 * local_heads, filled(low_part[at_moved]), aux)
                    aux = jnp.where(lane == TARGET_LANE, target_f, aux)
                    for j in range(local_heads):
                        rows_at = slice(
                            (t0 + j) * row_steps + h * half_rs,
                            (t0 + j) * row_steps + (h + 1) * half_rs,
                        )
                        aux = jnp.where(lane == j, top[rows_at], aux)
                        aux = jnp.where(lane == local_heads + j, top_part[rows_at], aux)
                        aux = jnp.where(lane == 2 * local_heads + j, low_part[rows_at], aux)
                    block = jnp.concatenate(parts + [filled(moved_acc), aux], axis=0)
                    dest = keep if side == 0 else send
                    dest[h, g * per_kv + kl] = block.astype(jnp.bfloat16)
        return carry

    lax.fori_loop(0, KVH, per_head, 0, unroll=UNROLL)
    for c in copies:
        c.wait()


def merge_kernel(local_heads, first, second, out):
    half_rs = (first.shape[2]) // (local_heads + 2)
    span = half_rs * local_heads
    lane = iota((half_rs, HD), 1)
    for h in range(first.shape[0]):
        for k in range(first.shape[1]):
            a = first[h, k].astype(jnp.float32)
            b = second[h, k].astype(jnp.float32)
            aux_a, aux_b = a[span + half_rs :], b[span + half_rs :]
            top = jnp.maximum(aux_a, aux_b)
            wa = jnp.exp2(aux_a - top)
            wb = jnp.exp2(aux_b - top)
            total = wa * sums_of(aux_a, local_heads) + wb * sums_of(aux_b, local_heads)
            high, low = split(total)
            is_top = (lane < local_heads) | (lane >= MOVED_LANE)
            is_top = is_top & (lane < MOVED_LANE + local_heads) | (lane == TARGET_LANE)
            high = pltpu.roll(high, local_heads, 1)
            low = pltpu.roll(low, 2 * local_heads, 1)
            part = lane % MOVED_LANE // local_heads
            aux = jnp.where(is_top, top, jnp.where(part == 1, high, low))
            parts = []
            for j in range(local_heads + 1):
                at = j if j < local_heads else MOVED_LANE
                rows = slice(j * half_rs, (j + 1) * half_rs)
                parts.append(wa[:, at : at + 1] * a[rows] + wb[:, at : at + 1] * b[rows])
            out[h, k] = jnp.concatenate(parts + [aux], axis=0).astype(jnp.bfloat16)


def reduce_kernel(chips, steps, info, parts, out):
    half_rs = out.shape[2]
    local_heads = out.shape[3] // HD
    half = info[0]
    span = half_rs * local_heads
    row_ids = iota((half_rs, 1), 0)
    tops, sums, accs = [], [], []
    for g in range(2):
        aux = [
            parts[g * chips + k, span + half_rs :].astype(jnp.float32) for k in range(chips)
        ]
        top = aux[0]
        for a in aux[1:]:
            top = jnp.maximum(top, a)
        total = None
        acc = [None] * (local_heads + 1)
        for k in range(chips):
            w = jnp.exp2(aux[k] - top)
            part = w * sums_of(aux[k], local_heads)
            total = part if total is None else total + part
            for j in range(local_heads + 1):
                at = j if j < local_heads else MOVED_LANE
                block = parts[g * chips + k, j * half_rs : (j + 1) * half_rs]
                part = w[:, at : at + 1] * block.astype(jnp.float32)
                acc[j] = part if acc[j] is None else acc[j] + part
        tops.append(top)
        sums.append(total)
        accs.append(acc)
    for g in range(2):
        slot = tops[1 - g][:, TARGET_LANE : TARGET_LANE + 1]
        mine = (half_rs // steps * half + row_ids // steps).astype(jnp.float32) == slot
        moved_top = tops[1 - g][:, MOVED_LANE : MOVED_LANE + 1]
        moved_sum = sums[1 - g][:, MOVED_LANE : MOVED_LANE + 1]
        moved_acc = accs[1 - g][local_heads]
        done = []
        for j in range(local_heads):

            def placed(x):
                y = jnp.broadcast_to(x[j * steps : j * steps + 1], (half_rs, x.shape[1]))
                for s in range(1, steps):
                    z = jnp.broadcast_to(x[j * steps + s : j * steps + s + 1], y.shape)
                    y = jnp.where(row_ids % steps == s, z, y)
                return y

            own_top = tops[g][:, j : j + 1]
            in_top = jnp.where(mine, placed(moved_top), FLOOR)
            top = jnp.maximum(own_top, in_top)
            w_own = jnp.exp2(own_top - top)
            w_in = jnp.where(mine, jnp.exp2(in_top - top), 0.0)
            total = w_own * sums[g][:, j : j + 1] + w_in * placed(moved_sum)
            done.append((w_own * accs[g][j] + w_in * placed(moved_acc)) / total)
        result = jnp.concatenate(done, axis=1).astype(jnp.bfloat16)
        for k in range(chips):
            out[g, k] = result


def project(chips, which, source, weight):
    acc = None
    for k in range(chips):
        x = jnp.concatenate([source[k], source[chips + k]], axis=0)
        part = dot(x, weight[2 * k + which], ((1,), (0,)))
        acc = part if acc is None else acc + part
    return acc


def project_own_kernel(chips, info, own, weight, out):
    out[...] = project(chips, info[1], own, weight)


def project_other_kernel(chips, info, partial, other, weight, out):
    total = partial[...] + project(chips, 1 - info[1], other, weight)
    out[...] = total.astype(jnp.bfloat16).reshape(out.shape)


def in_hbm(x):
    return pltpu.with_memory_space_constraint(x, pltpu.HBM)


def limit(mib):
    return pltpu.CompilerParams(vmem_limit_bytes=mib << 20)


SMEM = pl.BlockSpec(memory_space=pltpu.SMEM)
VMEM = pl.BlockSpec(memory_space=pltpu.VMEM)
HBM = pl.BlockSpec(memory_space=pltpu.HBM)
ANY = pl.BlockSpec(memory_space=pl.ANY)


def per_device_of(groups, width):
    chips = width // 2
    apart = groups // 2
    same_core = [
        [(g + h * apart) * width + 2 * k + c for h in range(2) for k in range(chips)]
        for g in range(apart)
        for c in range(2)
    ]
    across = [(t, t ^ 1) for t in range(width)]
    both = ("group", "tp")

    def exchange(x, members):
        return lax.all_to_all(x, both, 0, 0, axis_index_groups=members)

    def per_device(
        queries,
        new_keys,
        new_values,
        key_pages,
        value_pages,
        page_owner,
        page_fill,
        target_slot,
        out_weight,
    ):
        rows, steps, features = queries.shape[1:]
        local_heads = features // HD
        row_steps = rows * steps
        half_rs = row_steps // 2
        pages = key_pages.shape[1]
        tokens = pages * PAGE
        place = lax.axis_index("tp")
        half = lax.axis_index("group") // apart
        spread = width // KVH
        info = jnp.stack([half, place & 1, place & (spread - 1), place // spread])
        info = info.astype(jnp.int32)

        sent, new_own = pl.pallas_call(
            pack_kernel,
            out_shape=(
                jax.ShapeDtypeStruct((2 * chips, row_steps, features), jnp.bfloat16),
                jax.ShapeDtypeStruct((row_steps, 2 * new_keys.shape[3]), jnp.bfloat16),
            ),
            in_specs=[HBM] * 3,
            out_specs=(VMEM, VMEM),
            scratch_shapes=[
                pltpu.VMEM(x.shape[1:], x.dtype) for x in (queries, new_keys, new_values)
            ]
            + [pltpu.SemaphoreType.DMA((3,))],
            compiler_params=limit(4),
            name="pack",
        )(*(in_hbm(x[0]) for x in (queries, new_keys, new_values)))
        new_tokens = [new_own] + [
            lax.ppermute(new_own, "tp", [(t, t ^ i) for t in range(width)])
            for i in range(1, spread)
        ]
        own = exchange(sent, same_core)
        other = lax.ppermute(own, "tp", across)

        block_rows = half_rs * local_heads + 2 * half_rs
        state = jax.ShapeDtypeStruct((2, chips, block_rows, HD), jnp.bfloat16)
        ints = (target_slot, page_owner, page_fill)
        pages_shape = (tokens, key_pages.shape[3])
        keys, values, bias_own, bias_moved = pl.pallas_call(
            lambda *refs: prepare_kernel(steps, *refs),
            out_shape=(
                jax.ShapeDtypeStruct(pages_shape, key_pages.dtype),
                jax.ShapeDtypeStruct(pages_shape, value_pages.dtype),
                jax.ShapeDtypeStruct((row_steps, tokens), jnp.float32),
                jax.ShapeDtypeStruct((GS * steps, tokens), jnp.float32),
            ),
            in_specs=[HBM] * 5 + [ANY],
            out_specs=(VMEM,) * 4,
            scratch_shapes=[
                pltpu.SMEM(target_slot.shape, jnp.int32),
                pltpu.VMEM(page_owner.shape, jnp.int32),
                pltpu.VMEM(page_fill.shape, jnp.int32),
                pltpu.SemaphoreType.DMA((5,)),
            ],
            compiler_params=limit(8),
            name="prepare",
        )(
            *(in_hbm(x) for x in ints),
            in_hbm(key_pages.reshape(pages_shape)),
            in_hbm(value_pages.reshape(pages_shape)),
            own,
        )
        weight_by_device = out_weight.reshape(width, features, out_weight.shape[1])
        keep, send, weight = pl.pallas_call(
            lambda *refs: attend_kernel(chips, *refs),
            out_shape=(
                state,
                state,
                jax.ShapeDtypeStruct(weight_by_device.shape, weight_by_device.dtype),
            ),
            in_specs=[SMEM, SMEM] + [VMEM] * 6 + [HBM] + [VMEM] * spread,
            out_specs=(VMEM, VMEM, VMEM),
            scratch_shapes=[pltpu.SemaphoreType.DMA((width,))],
            compiler_params=limit(24),
            name="attend",
        )(
            info,
            target_slot,
            own,
            other,
            keys,
            values,
            bias_own,
            bias_moved,
            in_hbm(weight_by_device),
            *new_tokens,
        )
        merged = pl.pallas_call(
            lambda *refs: merge_kernel(local_heads, *refs),
            out_shape=state,
            in_specs=[VMEM, VMEM],
            out_specs=VMEM,
            compiler_params=limit(4),
            name="merge",
        )(keep, lax.ppermute(send, "tp", across))
        arrived = exchange(merged.reshape(2 * chips, block_rows, HD), same_core)
        finished = pl.pallas_call(
            lambda *refs: reduce_kernel(chips, steps, *refs),
            out_shape=jax.ShapeDtypeStruct((2, chips, half_rs, features), jnp.bfloat16),
            in_specs=[SMEM, VMEM],
            out_specs=VMEM,
            compiler_params=limit(4),
            name="reduce",
        )(info, arrived)
        own = exchange(finished.reshape(2 * chips, half_rs, features), same_core)
        other = lax.ppermute(own, "tp", across)
        partial = pl.pallas_call(
            lambda *refs: project_own_kernel(chips, *refs),
            out_shape=jax.ShapeDtypeStruct((row_steps, out_weight.shape[1]), jnp.float32),
            in_specs=[SMEM, VMEM, VMEM],
            out_specs=VMEM,
            compiler_params=limit(16),
            name="project_own",
        )(info, own, weight)
        projected = pl.pallas_call(
            lambda *refs: project_other_kernel(chips, *refs),
            out_shape=jax.ShapeDtypeStruct((rows, steps, out_weight.shape[1]), jnp.bfloat16),
            in_specs=[SMEM, VMEM, VMEM, VMEM],
            out_specs=VMEM,
            compiler_params=limit(16),
            name="project_other",
        )(info, partial, other, weight)
        return projected[None]

    return per_device


def solution(mesh):
    placed = (
        P("group", None, None, "tp"),
        P("group", None, None, "tp"),
        P("group", None, None, "tp"),
        P("group", "tp", None, None),
        P("group", "tp", None, None),
        P("group", "tp"),
        P("group", "tp"),
        P("group", None),
        P(None, "tp"),
    )
    return jax.shard_map(
        per_device_of(mesh.shape["group"], mesh.shape["tp"]),
        mesh=mesh,
        in_specs=placed,
        out_specs=P("group", None, None, "tp"),
        check_vma=False,
    )
```

```python
import math

import jax
import jax.numpy as jnp
from jax import lax
from jax.experimental import pallas as pl
from jax.experimental.pallas import tpu as pltpu
from jax.sharding import PartitionSpec as P

HEADS = 64
KVH = 8
HD = 128
PAGE = 16
NEG = -1e30
FLOOR = -1e29
SCALE = 1.0 / math.sqrt(HD) * math.log2(math.e)
MOVED_LANE = 64
TARGET_LANE = 127
GS = HEADS // KVH
UNROLL = 2
TOGETHER = 2
MERGE_UNROLL = 4
REDUCE_UNROLL = 2


def dot(a, b, contract):
    return lax.dot_general(a, b, ((contract), ((), ())), preferred_element_type=jnp.float32)


def iota(shape, axis):
    return lax.broadcasted_iota(jnp.int32, shape, axis)


def pack_kernel(queries, new_keys, new_values, out, new_out, q_buf, k_buf, v_buf, sems):
    row_steps = out.shape[1]
    buffers = (q_buf, k_buf, v_buf)
    copies = [
        pltpu.make_async_copy(x, b, sems.at[i])
        for i, (x, b) in enumerate(zip((queries, new_keys, new_values), buffers))
    ]
    for c in copies:
        c.start()
    for c in copies:
        c.wait()
    rows = [b[...].reshape(row_steps, b.shape[2]) for b in buffers]
    for i in range(out.shape[0]):
        out[i] = rows[0]
    new_out[...] = jnp.concatenate(rows[1:], axis=1)


def sums_of(aux, local_heads):
    high = pltpu.roll(aux, HD - local_heads, 1)
    return high + pltpu.roll(aux, HD - 2 * local_heads, 1)


def split(total):
    high = total.astype(jnp.bfloat16).astype(jnp.float32)
    return high, total - high


def mover_of(slots):
    rows = slots.shape[1]
    mover = jnp.int32(0)
    target = jnp.int32(0)
    for r in range(rows):
        leaves = slots[0, r] < rows
        mover = jnp.where(leaves, r, mover)
        target = jnp.where(leaves, slots[0, r], target)
    return mover, target


def prepare_kernel(
    steps,
    slots_hbm,
    owner_hbm,
    fill_hbm,
    keys_hbm,
    values_hbm,
    after,
    keys,
    values,
    bias_own,
    bias_moved,
    slots,
    owner,
    fill,
    sems,
):
    del after
    rows = slots.shape[1]
    row_steps, tokens = bias_own.shape
    sources = (slots_hbm, owner_hbm, fill_hbm, keys_hbm, values_hbm)
    targets = (slots, owner, fill, keys, values)
    copies = [
        pltpu.make_async_copy(source, target, sems.at[i])
        for i, (source, target) in enumerate(zip(sources, targets))
    ]
    for c in copies:
        c.start()
    for c in copies[:3]:
        c.wait()
    mover, _ = mover_of(slots)
    pages = owner.shape[1]
    spread = (iota((pages, tokens), 1) // PAGE == iota((pages, tokens), 0)).astype(jnp.bfloat16)
    table = jnp.concatenate([owner[...], fill[...]], axis=0).astype(jnp.float32)
    table = jnp.concatenate([table] * 4, axis=0).astype(jnp.bfloat16)
    by_token = dot(table, spread, ((1,), (0,)))
    owner_tok = by_token[0:1].astype(jnp.int32)
    fill_tok = by_token[1:2].astype(jnp.int32)
    live = iota((1, tokens), 1) % PAGE < fill_tok
    token_row = jnp.where(live, owner_tok, rows)
    stay_row = jnp.where(token_row == mover, rows, token_row)
    bias_own[...] = jnp.where(iota((row_steps, tokens), 0) // steps == stay_row, 0.0, NEG)
    bias_moved[...] = jnp.broadcast_to(jnp.where(token_row == mover, 0.0, NEG), bias_moved.shape)
    for c in copies[3:]:
        c.wait()


def attend_kernel(
    chips,
    info,
    slots,
    own,
    other,
    keys,
    values,
    bias_own,
    bias_moved,
    weight_hbm,
    *rest,
):
    *new_tokens, keep, send, weight, weight_sems = rest
    row_steps = own.shape[1]
    steps = row_steps // slots.shape[1]
    features = HEADS // (2 * chips) * HD
    local_heads = features // HD
    kv_part = new_tokens[0].shape[1] // 2
    per_kv = chips // KVH
    half_rs = row_steps // 2
    half = info[0]
    spot = info[2]
    own_kv = info[3]
    _, target = mover_of(slots)
    copies = [
        pltpu.make_async_copy(weight_hbm.at[i], weight.at[i], weight_sems.at[i])
        for i in range(weight.shape[0])
    ]
    for c in copies:
        c.start()

    rs_ids = iota((row_steps, row_steps), 0)
    new_ids = iota((row_steps, row_steps), 1)
    new_live = (rs_ids // steps == new_ids // steps) & (new_ids % steps <= rs_ids % steps)
    bias_new = jnp.where(new_live & (spot == 0), 0.0, NEG)
    pieces = []
    for p in range(len(new_tokens)):
        piece = new_tokens[0][...].astype(jnp.float32)
        for i in range(1, len(new_tokens)):
            piece = jnp.where(spot == p ^ i, new_tokens[i][...].astype(jnp.float32), piece)
        pieces.append(piece)
    new_k = jnp.concatenate([x[:, :kv_part] for x in pieces], axis=1).astype(jnp.bfloat16)
    new_v = jnp.concatenate([x[:, kv_part:] for x in pieces], axis=1).astype(jnp.bfloat16)
    moved_rows = GS * steps
    wide = GS * row_steps
    pick_ids = iota((moved_rows, wide), 0)
    pick = (
        iota((moved_rows, wide), 1)
        == (pick_ids // steps) * row_steps + target * steps + pick_ids % steps
    ).astype(jnp.bfloat16)
    lane = iota((half_rs, HD), 1)
    target_f = target.astype(jnp.float32)

    pad = HD - row_steps
    new_k = jnp.concatenate([new_k, jnp.zeros((pad, HD), new_k.dtype)], axis=0)
    new_v = jnp.concatenate([new_v, jnp.zeros((pad, HD), new_v.dtype)], axis=0)
    bias_new = jnp.concatenate([bias_new, jnp.full((row_steps, pad), NEG, jnp.float32)], axis=1)

    def gather(g):
        tiles, partner_tiles = [], []
        for source in (own, other):
            for kl in range(per_kv):
                mine = source[half * chips + g * per_kv + kl]
                theirs = source[(1 - half) * chips + g * per_kv + kl]
                for j in range(local_heads):
                    tiles.append(mine[:, j * HD : (j + 1) * HD])
                    partner_tiles.append(theirs[:, j * HD : (j + 1) * HD])
        moved_q = dot(pick, jnp.concatenate(partner_tiles, axis=0), ((1,), (0,)))
        return jnp.concatenate(tiles + [moved_q.astype(jnp.bfloat16)], axis=0)

    def score(g, q):
        k = keys[:, pl.ds(pl.multiple_of(g * HD, HD), HD)]
        scores = dot(q, jnp.concatenate([k, new_k], axis=0), ((1,), (1,))) * SCALE
        extra = jnp.where(g == own_kv, bias_new, NEG)
        bias_rows = jnp.concatenate([bias_own[...], extra], axis=1)
        moved = jnp.concatenate([bias_moved[...], jnp.full((moved_rows, HD), NEG)], axis=1)
        return scores + jnp.concatenate([bias_rows] * GS + [moved], axis=0)

    def weigh(scores):
        top = jnp.max(scores, axis=1, keepdims=True)
        top = jnp.maximum(top, FLOOR).astype(jnp.bfloat16).astype(jnp.float32)
        p = jnp.exp2(scores - top).astype(jnp.bfloat16)
        return top, p, jnp.sum(p.astype(jnp.float32), axis=1, keepdims=True)

    def combine(g, p):
        v = values[:, pl.ds(pl.multiple_of(g * HD, HD), HD)]
        return dot(p, jnp.concatenate([v, new_v], axis=0), ((1,), (0,)))

    def emit(g, top, total, acc):
        top_part, low_part = split(total)
        for side in range(2):
            for kl in range(per_kv):
                t0 = (side * per_kv + kl) * local_heads
                at_moved = slice(wide + t0 * steps, wide + (t0 + local_heads) * steps)
                moved_acc = acc[at_moved]
                short = half_rs - local_heads * steps

                def filled(x):
                    if short == 0:
                        return x
                    return jnp.concatenate([x, jnp.zeros((short, x.shape[1]), x.dtype)], axis=0)

                for h in range(2):
                    parts = [
                        acc[(t0 + j) * row_steps + h * half_rs :][:half_rs]
                        for j in range(local_heads)
                    ]
                    aux = jnp.where(lane == MOVED_LANE, filled(top[at_moved]), 0.0)
                    aux = jnp.where(lane == MOVED_LANE + local_heads, filled(top_part[at_moved]), aux)
                    aux = jnp.where(lane == MOVED_LANE + 2 * local_heads, filled(low_part[at_moved]), aux)
                    aux = jnp.where(lane == TARGET_LANE, target_f, aux)
                    for j in range(local_heads):
                        rows_at = slice(
                            (t0 + j) * row_steps + h * half_rs,
                            (t0 + j) * row_steps + (h + 1) * half_rs,
                        )
                        aux = jnp.where(lane == j, top[rows_at], aux)
                        aux = jnp.where(lane == local_heads + j, top_part[rows_at], aux)
                        aux = jnp.where(lane == 2 * local_heads + j, low_part[rows_at], aux)
                    block = jnp.concatenate(parts + [filled(moved_acc), aux], axis=0)
                    dest = keep if side == 0 else send
                    dest[h, g * per_kv + kl] = block.astype(jnp.bfloat16)

    def some_heads(i, carry):
        heads = [i * TOGETHER + n for n in range(TOGETHER)]
        scores = [score(g, q) for g, q in zip(heads, [gather(g) for g in heads])]
        weighed = [weigh(x) for x in scores]
        accs = [combine(g, w[1]) for g, w in zip(heads, weighed)]
        for g, w, acc in zip(heads, weighed, accs):
            emit(g, w[0], w[2], acc)
        return carry

    lax.fori_loop(0, KVH // TOGETHER, some_heads, 0, unroll=UNROLL)
    for c in copies:
        c.wait()


def merge_kernel(local_heads, first, second, out):
    half_rs = (first.shape[2]) // (local_heads + 2)
    span = half_rs * local_heads
    lane = iota((half_rs, HD), 1)
    chips = first.shape[1]

    def one(i, carry):
        h, k = i // chips, lax.rem(i, chips)
        a = first[h, k].astype(jnp.float32)
        b = second[h, k].astype(jnp.float32)
        aux_a, aux_b = a[span + half_rs :], b[span + half_rs :]
        top = jnp.maximum(aux_a, aux_b)
        wa = jnp.exp2(aux_a - top)
        wb = jnp.exp2(aux_b - top)
        total = wa * sums_of(aux_a, local_heads) + wb * sums_of(aux_b, local_heads)
        high, low = split(total)
        is_top = (lane < local_heads) | (lane >= MOVED_LANE)
        is_top = is_top & (lane < MOVED_LANE + local_heads) | (lane == TARGET_LANE)
        high = pltpu.roll(high, local_heads, 1)
        low = pltpu.roll(low, 2 * local_heads, 1)
        part = lane % MOVED_LANE // local_heads
        aux = jnp.where(is_top, top, jnp.where(part == 1, high, low))
        parts = []
        for j in range(local_heads + 1):
            at = j if j < local_heads else MOVED_LANE
            rows = slice(j * half_rs, (j + 1) * half_rs)
            parts.append(wa[:, at : at + 1] * a[rows] + wb[:, at : at + 1] * b[rows])
        out[h, k] = jnp.concatenate(parts + [aux], axis=0).astype(jnp.bfloat16)
        return carry

    lax.fori_loop(0, first.shape[0] * chips, one, 0, unroll=MERGE_UNROLL)


def reduce_kernel(chips, steps, info, parts, out):
    half_rs = out.shape[2]
    local_heads = out.shape[3] // HD
    half = info[0]
    span = half_rs * local_heads
    row_ids = iota((half_rs, 1), 0)
    tops, sums, accs = [], [], []
    for g in range(2):
        aux = [
            parts[g * chips + k, span + half_rs :].astype(jnp.float32) for k in range(chips)
        ]
        top = aux[0]
        for a in aux[1:]:
            top = jnp.maximum(top, a)
        total = None
        acc = [None] * (local_heads + 1)
        for k in range(chips):
            w = jnp.exp2(aux[k] - top)
            part = w * sums_of(aux[k], local_heads)
            total = part if total is None else total + part
            for j in range(local_heads + 1):
                at = j if j < local_heads else MOVED_LANE
                block = parts[g * chips + k, j * half_rs : (j + 1) * half_rs]
                part = w[:, at : at + 1] * block.astype(jnp.float32)
                acc[j] = part if acc[j] is None else acc[j] + part
        tops.append(top)
        sums.append(total)
        accs.append(acc)
    for g in range(2):
        slot = tops[1 - g][:, TARGET_LANE : TARGET_LANE + 1]
        mine = (half_rs // steps * half + row_ids // steps).astype(jnp.float32) == slot
        moved_top = tops[1 - g][:, MOVED_LANE : MOVED_LANE + 1]
        moved_sum = sums[1 - g][:, MOVED_LANE : MOVED_LANE + 1]
        moved_acc = accs[1 - g][local_heads]
        done = []
        for j in range(local_heads):

            def placed(x):
                y = jnp.broadcast_to(x[j * steps : j * steps + 1], (half_rs, x.shape[1]))
                for s in range(1, steps):
                    z = jnp.broadcast_to(x[j * steps + s : j * steps + s + 1], y.shape)
                    y = jnp.where(row_ids % steps == s, z, y)
                return y

            own_top = tops[g][:, j : j + 1]
            in_top = jnp.where(mine, placed(moved_top), FLOOR)
            top = jnp.maximum(own_top, in_top)
            w_own = jnp.exp2(own_top - top)
            w_in = jnp.where(mine, jnp.exp2(in_top - top), 0.0)
            total = w_own * sums[g][:, j : j + 1] + w_in * placed(moved_sum)
            done.append((w_own * accs[g][j] + w_in * placed(moved_acc)) / total)
        result = jnp.concatenate(done, axis=1).astype(jnp.bfloat16)
        for k in range(chips):
            out[g, k] = result


def project(chips, which, source, weight):
    acc = None
    for k in range(chips):
        x = jnp.concatenate([source[k], source[chips + k]], axis=0)
        part = dot(x, weight[2 * k + which], ((1,), (0,)))
        acc = part if acc is None else acc + part
    return acc


def project_own_kernel(chips, info, own, weight, out):
    out[...] = project(chips, info[1], own, weight)


def project_other_kernel(chips, info, partial, other, weight, out):
    total = partial[...] + project(chips, 1 - info[1], other, weight)
    out[...] = total.astype(jnp.bfloat16).reshape(out.shape)


def in_hbm(x):
    return pltpu.with_memory_space_constraint(x, pltpu.HBM)


def limit(mib):
    return pltpu.CompilerParams(vmem_limit_bytes=mib << 20)


SMEM = pl.BlockSpec(memory_space=pltpu.SMEM)
VMEM = pl.BlockSpec(memory_space=pltpu.VMEM)
HBM = pl.BlockSpec(memory_space=pltpu.HBM)
ANY = pl.BlockSpec(memory_space=pl.ANY)


def per_device_of(groups, width):
    chips = width // 2
    apart = groups // 2
    same_core = [
        [(g + h * apart) * width + 2 * k + c for h in range(2) for k in range(chips)]
        for g in range(apart)
        for c in range(2)
    ]
    across = [(t, t ^ 1) for t in range(width)]
    both = ("group", "tp")

    def exchange(x, members):
        return lax.all_to_all(x, both, 0, 0, axis_index_groups=members)

    def per_device(
        queries,
        new_keys,
        new_values,
        key_pages,
        value_pages,
        page_owner,
        page_fill,
        target_slot,
        out_weight,
    ):
        rows, steps, features = queries.shape[1:]
        local_heads = features // HD
        row_steps = rows * steps
        half_rs = row_steps // 2
        pages = key_pages.shape[1]
        tokens = pages * PAGE
        place = lax.axis_index("tp")
        half = lax.axis_index("group") // apart
        spread = width // KVH
        info = jnp.stack([half, place & 1, place & (spread - 1), place // spread])
        info = info.astype(jnp.int32)

        sent, new_own = pl.pallas_call(
            pack_kernel,
            out_shape=(
                jax.ShapeDtypeStruct((2 * chips, row_steps, features), jnp.bfloat16),
                jax.ShapeDtypeStruct((row_steps, 2 * new_keys.shape[3]), jnp.bfloat16),
            ),
            in_specs=[HBM] * 3,
            out_specs=(VMEM, VMEM),
            scratch_shapes=[
                pltpu.VMEM(x.shape[1:], x.dtype) for x in (queries, new_keys, new_values)
            ]
            + [pltpu.SemaphoreType.DMA((3,))],
            compiler_params=limit(4),
            name="pack",
        )(*(in_hbm(x[0]) for x in (queries, new_keys, new_values)))
        new_tokens = [new_own] + [
            lax.ppermute(new_own, "tp", [(t, t ^ i) for t in range(width)])
            for i in range(1, spread)
        ]
        own = exchange(sent, same_core)
        other = lax.ppermute(own, "tp", across)

        block_rows = half_rs * local_heads + 2 * half_rs
        state = jax.ShapeDtypeStruct((2, chips, block_rows, HD), jnp.bfloat16)
        ints = (target_slot, page_owner, page_fill)
        pages_shape = (tokens, key_pages.shape[3])
        keys, values, bias_own, bias_moved = pl.pallas_call(
            lambda *refs: prepare_kernel(steps, *refs),
            out_shape=(
                jax.ShapeDtypeStruct(pages_shape, key_pages.dtype),
                jax.ShapeDtypeStruct(pages_shape, value_pages.dtype),
                jax.ShapeDtypeStruct((row_steps, tokens), jnp.float32),
                jax.ShapeDtypeStruct((GS * steps, tokens), jnp.float32),
            ),
            in_specs=[HBM] * 5 + [ANY],
            out_specs=(VMEM,) * 4,
            scratch_shapes=[
                pltpu.SMEM(target_slot.shape, jnp.int32),
                pltpu.VMEM(page_owner.shape, jnp.int32),
                pltpu.VMEM(page_fill.shape, jnp.int32),
                pltpu.SemaphoreType.DMA((5,)),
            ],
            compiler_params=limit(8),
            name="prepare",
        )(
            *(in_hbm(x) for x in ints),
            in_hbm(key_pages.reshape(pages_shape)),
            in_hbm(value_pages.reshape(pages_shape)),
            own,
        )
        weight_by_device = out_weight.reshape(width, features, out_weight.shape[1])
        keep, send, weight = pl.pallas_call(
            lambda *refs: attend_kernel(chips, *refs),
            out_shape=(
                state,
                state,
                jax.ShapeDtypeStruct(weight_by_device.shape, weight_by_device.dtype),
            ),
            in_specs=[SMEM, SMEM] + [VMEM] * 6 + [HBM] + [VMEM] * spread,
            out_specs=(VMEM, VMEM, VMEM),
            scratch_shapes=[pltpu.SemaphoreType.DMA((width,))],
            compiler_params=limit(24),
            name="attend",
        )(
            info,
            target_slot,
            own,
            other,
            keys,
            values,
            bias_own,
            bias_moved,
            in_hbm(weight_by_device),
            *new_tokens,
        )
        merged = pl.pallas_call(
            lambda *refs: merge_kernel(local_heads, *refs),
            out_shape=state,
            in_specs=[VMEM, VMEM],
            out_specs=VMEM,
            compiler_params=limit(4),
            name="merge",
        )(keep, lax.ppermute(send, "tp", across))
        arrived = exchange(merged.reshape(2 * chips, block_rows, HD), same_core)
        finished = pl.pallas_call(
            lambda *refs: reduce_kernel(chips, steps, *refs),
            out_shape=jax.ShapeDtypeStruct((2, chips, half_rs, features), jnp.bfloat16),
            in_specs=[SMEM, VMEM],
            out_specs=VMEM,
            compiler_params=limit(4),
            name="reduce",
        )(info, arrived)
        own = exchange(finished.reshape(2 * chips, half_rs, features), same_core)
        other = lax.ppermute(own, "tp", across)
        partial = pl.pallas_call(
            lambda *refs: project_own_kernel(chips, *refs),
            out_shape=jax.ShapeDtypeStruct((row_steps, out_weight.shape[1]), jnp.float32),
            in_specs=[SMEM, VMEM, VMEM],
            out_specs=VMEM,
            compiler_params=limit(16),
            name="project_own",
        )(info, own, weight)
        projected = pl.pallas_call(
            lambda *refs: project_other_kernel(chips, *refs),
            out_shape=jax.ShapeDtypeStruct((rows, steps, out_weight.shape[1]), jnp.bfloat16),
            in_specs=[SMEM, VMEM, VMEM, VMEM],
            out_specs=VMEM,
            compiler_params=limit(16),
            name="project_other",
        )(info, partial, other, weight)
        return projected[None]

    return per_device


def solution(mesh):
    placed = (
        P("group", None, None, "tp"),
        P("group", None, None, "tp"),
        P("group", None, None, "tp"),
        P("group", "tp", None, None),
        P("group", "tp", None, None),
        P("group", "tp"),
        P("group", "tp"),
        P("group", None),
        P(None, "tp"),
    )
    return jax.shard_map(
        per_device_of(mesh.shape["group"], mesh.shape["tp"]),
        mesh=mesh,
        in_specs=placed,
        out_specs=P("group", None, None, "tp"),
        check_vma=False,
    )
```
